8 devices in a mesh: pp: 2 (over z, y), ep: 4 (over x, core).
Axes of the slice: x: 2, y: 2, z: 1, core: 2. Of those that a mesh axis runs over, the one named last changes fastest.
Arguments:
- x_fwd: bfloat16 [2, 4096, 256], P('pp', 'ep')
- x_bwd: bfloat16 [2, 4096, 256], P('pp', 'ep')
- grad_in: bfloat16 [2, 4096, 256], P('pp', 'ep')
- dense_in: bfloat16 [2, 2, 256, 768], P('pp')
- dense_out: bfloat16 [2, 2, 768, 256], P('pp')
- exp_gate: bfloat16 [2, 2, 128, 256, 128], P('pp', None, 'ep')
- exp_up: bfloat16 [2, 2, 128, 256, 128], P('pp', None, 'ep')
- exp_down: bfloat16 [2, 2, 128, 128, 256], P('pp', None, 'ep')
- route_fwd: int32 [2, 2, 4096, 8], P('pp', None, 'ep')
- gate_fwd: bfloat16 [2, 2, 4096, 8], P('pp', None, 'ep')
- route_bwd: int32 [2, 2, 4096, 8], P('pp', None, 'ep')
- gate_bwd: bfloat16 [2, 2, 4096, 8], P('pp', None, 'ep')
Outputs:
- output 1: bfloat16 [2, 4096, 256], P('pp', 'ep')
- output 2: bfloat16 [2, 4096, 256], P('pp', 'ep')
- output 3: float32 [2, 2, 128, 256, 128], P('pp', None, 'ep')
- output 4: float32 [2, 2, 128, 256, 128], P('pp', None, 'ep')
- output 5: float32 [2, 2, 128, 128, 256], P('pp', None, 'ep')
All inputs are finite; a program needn't handle non-finite values.
Results may differ from the reference program's by a relative error of at most 0.0184101.
Values are sent between devices in bfloat16 or wider.
A program may use at most 1 GiB of HBM per device.

```python
import jax
import jax.numpy as jnp
from jax import lax

STAGES = 2
GROUPS = 4
TOKENS_DEV = 1024
HIDDEN = 256
DENSE_FF = 768
EXPERT_FF = 128
EXPERTS = 128
TOP_K = 8
CAPACITY = 2 * TOKENS_DEV * TOP_K // EXPERTS
NORM_EPS = 1e-6


def rms_norm(values):
    return values * lax.rsqrt(jnp.mean(values * values, axis=-1, keepdims=True) + NORM_EPS)


def rms_back(values, grad_out):
    inv_rms = lax.rsqrt(jnp.mean(values * values, axis=-1, keepdims=True) + NORM_EPS)
    proj_mean = jnp.mean(grad_out * values, axis=-1, keepdims=True)
    return inv_rms * grad_out - values * (inv_rms * inv_rms * inv_rms) * proj_mean


def silu_grad(pre_act):
    sig_value = jax.nn.sigmoid(pre_act)
    return sig_value * (1.0 + pre_act * (1.0 - sig_value))


def draw_route(key):
    key_order, key_shift, key_perm = jax.random.split(key, 3)
    half_cap = CAPACITY // 2
    expert_order = jax.random.permutation(key_order, EXPERTS)
    pair_shift = jax.random.randint(key_shift, (EXPERTS // 2,), 0, half_cap + 1).at[0].set(half_cap)
    counts = jnp.full((EXPERTS,), half_cap, jnp.int32).at[expert_order[0::2]].add(pair_shift).at[expert_order[1::2]].add(-pair_shift)
    run_ends = jnp.cumsum(counts)
    positions = jnp.arange(TOKENS_DEV * TOP_K, dtype=jnp.int32)
    expert_ids = jnp.searchsorted(run_ends, positions, side='right')
    slot_ids = positions - (run_ends - counts)[expert_ids]
    route_table = (expert_ids * CAPACITY + slot_ids).astype(jnp.int32).reshape(TOP_K, TOKENS_DEV).T
    return route_table[jax.random.permutation(key_perm, TOKENS_DEV)]


def draw_routes(key):
    keys = jax.random.split(key, STAGES * 2 * GROUPS)
    return jax.vmap(draw_route)(keys).reshape(STAGES, 2, GROUPS * TOKENS_DEV, TOP_K)


def setup_inputs(seed: int = 0) -> dict:
    keys = jax.random.split(jax.random.key(seed), 12)
    tok_shape = (STAGES, GROUPS * TOKENS_DEV, HIDDEN)
    route_shape = (STAGES, 2, GROUPS * TOKENS_DEV, TOP_K)
    up_shape = (STAGES, 2, EXPERTS, HIDDEN, EXPERT_FF)
    down_shape = (STAGES, 2, EXPERTS, EXPERT_FF, HIDDEN)

    def normal_bf16(key, shape, scale):
        return (jax.random.normal(key, shape, jnp.float32) * scale).astype(jnp.bfloat16)

    def gate_draw(key):
        return (jax.random.uniform(key, route_shape, jnp.float32, 0.05, 1.95) * (2.0 * TOP_K ** -0.5)).astype(jnp.bfloat16)

    return dict(
        x_fwd=normal_bf16(keys[0], tok_shape, 1.0),
        x_bwd=normal_bf16(keys[1], tok_shape, 1.0),
        grad_in=normal_bf16(keys[2], tok_shape, 1.0),
        dense_in=normal_bf16(keys[3], (STAGES, 2, HIDDEN, DENSE_FF), HIDDEN ** -0.5),
        dense_out=normal_bf16(keys[4], (STAGES, 2, DENSE_FF, HIDDEN), DENSE_FF ** -0.5),
        exp_gate=normal_bf16(keys[5], up_shape, HIDDEN ** -0.5),
        exp_up=normal_bf16(keys[6], up_shape, HIDDEN ** -0.5),
        exp_down=normal_bf16(keys[7], down_shape, EXPERT_FF ** -0.5),
        route_fwd=draw_routes(keys[8]),
        gate_fwd=gate_draw(keys[9]),
        route_bwd=draw_routes(keys[10]),
        gate_bwd=gate_draw(keys[11]),
    )


def to_slots(rows, route):
    def one_source(src_rows, src_route):
        table = jnp.zeros((EXPERTS * CAPACITY, HIDDEN), src_rows.dtype)
        return table.at[src_route.reshape(-1)].set(src_rows.reshape(-1, HIDDEN))
    return jax.vmap(one_source)(rows, route).reshape(GROUPS, EXPERTS, CAPACITY, HIDDEN)


def from_slots(table, route):
    flat = table.reshape(GROUPS, EXPERTS * CAPACITY, HIDDEN)
    return jax.vmap(lambda src_table, src_route: src_table[src_route])(flat, route)


def dense_forward(tokens, w_in, w_out):
    normed = rms_norm(tokens.astype(jnp.float32)).astype(jnp.bfloat16)
    pre_act = jnp.dot(normed, w_in, preferred_element_type=jnp.float32)
    mid_act = jax.nn.silu(pre_act).astype(jnp.bfloat16)
    hidden = (tokens.astype(jnp.float32) + jnp.dot(mid_act, w_out, preferred_element_type=jnp.float32)).astype(jnp.bfloat16)
    return pre_act, hidden


def block_front(tokens, route, weights):
    w_in, w_out, w_gate, w_up, w_down = weights
    flat = tokens.reshape(GROUPS * TOKENS_DEV, HIDDEN)
    pre_act, hidden = dense_forward(flat, w_in, w_out)
    normed = rms_norm(hidden.astype(jnp.float32)).astype(jnp.bfloat16)
    spread = jnp.broadcast_to(normed.reshape(GROUPS, TOKENS_DEV, 1, HIDDEN), (GROUPS, TOKENS_DEV, TOP_K, HIDDEN))
    slots = to_slots(spread, route).astype(jnp.float32)
    gate_pre = jnp.einsum('gecd,edf->gecf', slots, w_gate.astype(jnp.float32))
    up_pre = jnp.einsum('gecd,edf->gecf', slots, w_up.astype(jnp.float32))
    expert_mid = (jax.nn.silu(gate_pre) * up_pre).astype(jnp.bfloat16)
    return flat, pre_act, hidden, slots, gate_pre, up_pre, expert_mid


def block_finish(saved, route, gate, weights):
    hidden = saved[2]
    expert_mid = saved[6]
    expert_out = jnp.einsum('gecf,efd->gecd', expert_mid.astype(jnp.float32), weights[4].astype(jnp.float32)).astype(jnp.bfloat16)
    picked = from_slots(expert_out, route)
    mixed = jnp.einsum('gtk,gtkd->gtd', gate.astype(jnp.float32), picked.astype(jnp.float32))
    return (hidden.reshape(GROUPS, TOKENS_DEV, HIDDEN).astype(jnp.float32) + mixed).astype(jnp.bfloat16)


def block_backward(grad_out, saved, route, gate, weights):
    w_in, w_out, w_gate, w_up, w_down = weights
    flat, pre_act, hidden, slots, gate_pre, up_pre, expert_mid = saved
    grad_send = (gate.astype(jnp.float32)[..., None] * grad_out.astype(jnp.float32)[:, :, None, :]).astype(jnp.bfloat16)
    grad_slots = to_slots(grad_send, route).astype(jnp.float32)
    grad_mid = jnp.einsum('gecd,efd->gecf', grad_slots, w_down.astype(jnp.float32))
    grad_gate_pre = (grad_mid * up_pre * silu_grad(gate_pre)).astype(jnp.bfloat16).astype(jnp.float32)
    grad_up_pre = (grad_mid * jax.nn.silu(gate_pre)).astype(jnp.bfloat16).astype(jnp.float32)
    dw_down = jnp.einsum('gecf,gecd->efd', expert_mid.astype(jnp.float32), grad_slots)
    dw_gate = jnp.einsum('gecd,gecf->edf', slots, grad_gate_pre)
    dw_up = jnp.einsum('gecd,gecf->edf', slots, grad_up_pre)
    grad_rows = (jnp.einsum('gecf,edf->gecd', grad_gate_pre, w_gate.astype(jnp.float32)) + jnp.einsum('gecf,edf->gecd', grad_up_pre, w_up.astype(jnp.float32))).astype(jnp.bfloat16)
    grad_norm = jnp.sum(from_slots(grad_rows, route).astype(jnp.float32), axis=2).reshape(GROUPS * TOKENS_DEV, HIDDEN)
    grad_hidden = grad_out.reshape(GROUPS * TOKENS_DEV, HIDDEN).astype(jnp.float32) + rms_back(hidden.astype(jnp.float32), grad_norm)
    grad_dense = jnp.dot(grad_hidden.astype(jnp.bfloat16), w_out.T, preferred_element_type=jnp.float32)
    grad_pre = (grad_dense * silu_grad(pre_act)).astype(jnp.bfloat16)
    grad_act = jnp.dot(grad_pre, w_in.T, preferred_element_type=jnp.float32)
    grad_tokens = (grad_hidden + rms_back(flat.astype(jnp.float32), grad_act)).astype(jnp.bfloat16)
    return grad_tokens.reshape(GROUPS, TOKENS_DEV, HIDDEN), dw_gate, dw_up, dw_down


def stage_step(operands):
    x_fwd, x_bwd, grad_in, dense_in, dense_out, exp_gate, exp_up, exp_down, route_fwd, gate_fwd, route_bwd, gate_bwd = operands
    tok_shape = (GROUPS, TOKENS_DEV, HIDDEN)
    route_shape = (2, GROUPS, TOKENS_DEV, TOP_K)
    route_f = route_fwd.reshape(route_shape)
    gate_f = gate_fwd.reshape(route_shape)
    route_b = route_bwd.reshape(route_shape)
    gate_b = gate_bwd.reshape(route_shape)
    weights = [(dense_in[block], dense_out[block], exp_gate[block], exp_up[block], exp_down[block]) for block in range(2)]
    tokens = x_fwd.reshape(tok_shape)
    for block in range(2):
        saved = block_front(tokens, route_f[block], weights[block])
        tokens = block_finish(saved, route_f[block], gate_f[block], weights[block])
    saved_first = block_front(x_bwd.reshape(tok_shape), route_b[0], weights[0])
    mid_tokens = block_finish(saved_first, route_b[0], gate_b[0], weights[0])
    saved_second = block_front(mid_tokens, route_b[1], weights[1])
    grad_mid, wg_two, wu_two, wd_two = block_backward(grad_in.reshape(tok_shape), saved_second, route_b[1], gate_b[1], weights[1])
    grad_first, wg_one, wu_one, wd_one = block_backward(grad_mid, saved_first, route_b[0], gate_b[0], weights[0])
    return (tokens.reshape(GROUPS * TOKENS_DEV, HIDDEN), grad_first.reshape(GROUPS * TOKENS_DEV, HIDDEN), jnp.stack([wg_one, wg_two]), jnp.stack([wu_one, wu_two]), jnp.stack([wd_one, wd_two]))


def reference(x_fwd, x_bwd, grad_in, dense_in, dense_out, exp_gate, exp_up, exp_down, route_fwd, gate_fwd, route_bwd, gate_bwd):
    results = lax.map(stage_step, (x_fwd, x_bwd, grad_in, dense_in, dense_out, exp_gate, exp_up, exp_down, route_fwd, gate_fwd, route_bwd, gate_bwd))
    y_out, dx_out, dw_gate, dw_up, dw_down = results
    return jnp.roll(y_out, 1, axis=0), jnp.roll(dx_out, -1, axis=0), dw_gate, dw_up, dw_down
```

```python
import functools

import jax
import jax.numpy as jnp
from jax import lax
from jax.experimental import pallas as pl
from jax.experimental.pallas import tpu as pltpu
from jax.sharding import PartitionSpec as P

NORM_EPS = 1e-6
WIN = 16
TILE = 256
CHUNK = 16
MAIN = 4

f32 = jnp.float32
bf16 = jnp.bfloat16


def rms_norm(values):
    return values * lax.rsqrt(jnp.mean(values * values, axis=-1, keepdims=True) + NORM_EPS)


def rms_back(values, grad_out):
    inv_rms = lax.rsqrt(jnp.mean(values * values, axis=-1, keepdims=True) + NORM_EPS)
    proj_mean = jnp.mean(grad_out * values, axis=-1, keepdims=True)
    return inv_rms * grad_out - values * (inv_rms * inv_rms * inv_rms) * proj_mean


def silu_grad(pre_act):
    sig_value = jax.nn.sigmoid(pre_act)
    return sig_value * (1.0 + pre_act * (1.0 - sig_value))


def dense_forward(tokens, w_in, w_out):
    normed = rms_norm(tokens.astype(f32)).astype(bf16)
    pre_act = jnp.dot(normed, w_in, preferred_element_type=f32)
    mid_act = jax.nn.silu(pre_act).astype(bf16)
    hidden = (tokens.astype(f32) + jnp.dot(mid_act, w_out, preferred_element_type=f32)).astype(bf16)
    return pre_act, hidden


def dense_backward(grad_hidden, tokens, pre_act, w_in, w_out):
    grad_dense = jnp.einsum('td,fd->tf', grad_hidden.astype(bf16), w_out, preferred_element_type=f32)
    grad_pre = (grad_dense * silu_grad(pre_act)).astype(bf16)
    grad_act = jnp.einsum('tf,df->td', grad_pre, w_in, preferred_element_type=f32)
    return (grad_hidden + rms_back(tokens.astype(f32), grad_act)).astype(bf16)


class Plan:
    def __init__(self, n_tok, groups, experts, choices, width, ff):
        self.n_tok, self.groups, self.experts, self.width, self.ff = n_tok, groups, experts, width, ff
        self.total = n_tok * groups
        self.tiles = self.total // TILE
        capacity = 2 * n_tok * choices // (experts * groups)
        worst = (TILE * choices + experts * (WIN - 1)) // WIN
        self.per_tile = -(-worst // CHUNK) * CHUNK
        self.per_exp = -(-(groups * capacity + self.tiles * (WIN - 1)) // (WIN * 16)) * 16
        self.rows = self.per_exp * WIN
        self.trash = experts * self.per_exp
        self.buf_rows = (self.trash + 1) * WIN


def one_hot_rows(plan, tab, lr, gt, tile, chunk, plain, gated):
    win_exp, win_base = tab
    lane = pl.ds(pl.multiple_of(tile * TILE, TILE), TILE)
    iota = lax.broadcasted_iota(jnp.int32, (WIN, TILE), 0)
    ones, gates = [], []
    for i in range(CHUNK):
        spot = tile * plan.per_tile + chunk * CHUNK + i
        exp = win_exp[spot]
        hit = (lr[pl.ds(exp, 1), lane] - win_base[spot]) == iota
        if plain:
            ones.append(jnp.where(hit, 1.0, 0.0).astype(bf16))
        if gated:
            gates.append(jnp.where(hit, gt[pl.ds(exp, 1), lane], 0.0).astype(bf16))
    return (jnp.concatenate(ones, 0) if plain else None), (jnp.concatenate(gates, 0) if gated else None)


def win_rows(plan, win_dst, tile, chunk, i):
    dst = win_dst[tile * plan.per_tile + chunk * CHUNK + i]
    return pl.ds(pl.multiple_of(dst * WIN, WIN), WIN)


def dot(a, b):
    return jnp.dot(a, b, preferred_element_type=f32)


def dot_tb(a, b):
    return lax.dot_general(a, b, (((1,), (1,)), ((), ())), preferred_element_type=f32)


def dot_ta(a, b):
    return lax.dot_general(a, b, (((0,), (0,)), ((), ())), preferred_element_type=f32)


def combine_tile(plan, tab, win_dst, win_chunks, lr, gt, tile, buf, out, gated):
    def piece(chunk):
        ones, gates = one_hot_rows(plan, tab, lr, gt, tile, chunk, not gated, gated)
        rows = jnp.concatenate([buf[win_rows(plan, win_dst, tile, chunk, i), :] for i in range(CHUNK)], 0)
        return dot_ta(gates if gated else ones, rows)

    total = piece(0)
    for chunk in range(1, MAIN):
        total = total + piece(chunk)
    span = pl.ds(pl.multiple_of(tile * TILE, TILE), TILE)
    out[span, :] = total

    def more(chunk, _):
        out[span, :] += piece(chunk)
        return 0

    lax.fori_loop(MAIN, jnp.maximum(win_chunks[tile], MAIN), more, 0)


def forward_kernel(plan, win_exp, win_base, win_dst, win_chunks, exp_wins, lr, gt, z0, z1, z2, wg_in, wu_in, wd_in, y_near, y_far, z, wg, wu, wd, buf, y, sems):
    n_tok = plan.n_tok
    pieces = [(z0, pl.ds(0, n_tok)), (z1, pl.ds(n_tok, n_tok)), (z2, pl.ds(2 * n_tok, 2 * n_tok))]
    loads = [pltpu.make_async_copy(src, z.at[dst], sems.at[i]) for i, (src, dst) in enumerate(pieces)]
    loads += [pltpu.make_async_copy(src, dst, sems.at[3 + i]) for i, (src, dst) in enumerate([(wg_in, wg), (wu_in, wu), (wd_in, wd)])]
    for load in loads:
        load.start()
    tab = (win_exp, win_base)
    for load in loads[:3]:
        load.wait()

    def dispatch(tile, _):
        rows = z[pl.ds(pl.multiple_of(tile * TILE, TILE), TILE), :]

        def piece(chunk):
            ones, _ = one_hot_rows(plan, tab, lr, gt, tile, chunk, True, False)
            moved = dot(ones, rows).astype(bf16)
            for i in range(CHUNK):
                buf[win_rows(plan, win_dst, tile, chunk, i), :] = moved[i * WIN:(i + 1) * WIN, :]

        for chunk in range(MAIN):
            piece(chunk)

        def more(chunk, _):
            piece(chunk)
            return 0

        lax.fori_loop(MAIN, jnp.maximum(win_chunks[tile], MAIN), more, 0)
        return 0

    lax.fori_loop(0, plan.tiles, dispatch, 0)
    for load in loads[3:]:
        load.wait()

    def expert(exp, _):
        w_in = jnp.concatenate([wg[exp], wu[exp]], 1)
        w_out = wd[exp]

        def part(first):
            span = pl.ds(pl.multiple_of(exp * plan.rows + first, TILE), TILE)
            pre = dot(buf[span, :], w_in)
            mid = (jax.nn.silu(pre[:, :plan.ff]) * pre[:, plan.ff:]).astype(bf16)
            buf[span, :] = dot(mid, w_out).astype(bf16)

        part(0)
        part(TILE)
        for first in range(2 * TILE, plan.rows, TILE):
            @pl.when(exp_wins[exp] * WIN > first)
            def _(first=first):
                part(first)
        return 0

    lax.fori_loop(0, plan.experts, expert, 0)

    def combine(tile, _):
        combine_tile(plan, tab, win_dst, win_chunks, lr, gt, tile, buf, y, True)
        return 0

    half = plan.tiles // 2
    lax.fori_loop(half, plan.tiles, combine, 0)
    far = pltpu.make_async_copy(y.at[pl.ds(2 * n_tok, 2 * n_tok)], y_far, sems.at[0])
    far.start()
    lax.fori_loop(0, half, combine, 0)
    near = pltpu.make_async_copy(y.at[pl.ds(0, 2 * n_tok)], y_near, sems.at[1])
    near.start()
    far.wait()
    near.wait()


def backward_kernel(plan, win_exp, win_base, win_dst, win_chunks, exp_wins, lr, gt, z0, z1, z2, g0, g1, g2, wg_in, wu_in, wd_in, y_near, y_far, dwg, dwu, dwd, zg, wg, wu, wd, buf, rbuf, y, ogu, od, sems, osems):
    n_tok, width, ff = plan.n_tok, plan.width, plan.ff
    loads = []
    for col, group in ((0, (z0, z1, z2)), (1, (g0, g1, g2))):
        for i, src in enumerate(group):
            dst = zg.at[col, pl.ds(i * n_tok, n_tok if i < 2 else 2 * n_tok)]
            loads.append(pltpu.make_async_copy(src, dst, sems.at[len(loads)]))
    loads += [pltpu.make_async_copy(src, dst, sems.at[6 + i]) for i, (src, dst) in enumerate([(wg_in, wg), (wu_in, wu), (wd_in, wd)])]
    for load in loads:
        load.start()
    tab = (win_exp, win_base)

    def clear(step, _):
        span = pl.ds(pl.multiple_of(step * TILE, TILE), TILE)
        buf[span, :] = jnp.zeros((TILE, width), bf16)
        rbuf[span, :] = jnp.zeros((TILE, width), bf16)
        return 0

    lax.fori_loop(0, plan.experts * plan.rows // TILE, clear, 0)
    for load in loads[:6]:
        load.wait()

    def dispatch(tile, _):
        span = pl.ds(pl.multiple_of(tile * TILE, TILE), TILE)
        z_rows, g_rows = zg[0, span, :], zg[1, span, :]

        def piece(chunk):
            ones, gates = one_hot_rows(plan, tab, lr, gt, tile, chunk, True, True)
            moved = dot(ones, z_rows).astype(bf16)
            sent = dot(gates, g_rows).astype(bf16)
            for i in range(CHUNK):
                dst = win_rows(plan, win_dst, tile, chunk, i)
                buf[dst, :] = moved[i * WIN:(i + 1) * WIN, :]
                rbuf[dst, :] = sent[i * WIN:(i + 1) * WIN, :]

        for chunk in range(MAIN):
            piece(chunk)

        def more(chunk, _):
            piece(chunk)
            return 0

        lax.fori_loop(MAIN, jnp.maximum(win_chunks[tile], MAIN), more, 0)
        return 0

    lax.fori_loop(0, plan.tiles, dispatch, 0)
    for load in loads[6:]:
        load.wait()

    def stores(exp, slot):
        return [
            pltpu.make_async_copy(ogu.at[slot, 0], dwg.at[exp], osems.at[slot, 0]),
            pltpu.make_async_copy(ogu.at[slot, 1], dwu.at[exp], osems.at[slot, 1]),
            pltpu.make_async_copy(od.at[slot], dwd.at[exp], osems.at[slot, 2]),
        ]

    def expert(exp, _):
        slot = lax.rem(exp, 2)

        @pl.when(exp >= 2)
        def _():
            for store in stores(exp - 2, slot):
                store.wait()

        w_in = jnp.concatenate([wg[exp], wu[exp]], 1)
        w_out = wd[exp]

        def part(first):
            span = pl.ds(pl.multiple_of(exp * plan.rows + first, TILE), TILE)
            x, r = buf[span, :], rbuf[span, :]
            pre = dot(x, w_in)
            gate_pre, up_pre = pre[:, :ff], pre[:, ff:]
            sig = jax.nn.sigmoid(gate_pre)
            act = gate_pre * sig
            mid = (act * up_pre).astype(bf16)
            grad_mid = dot_tb(r, w_out)
            grad_gate = (grad_mid * up_pre * (sig * (1.0 + gate_pre * (1.0 - sig)))).astype(bf16)
            grad_up = (grad_mid * act).astype(bf16)
            both = jnp.concatenate([grad_gate, grad_up], 1)
            buf[span, :] = dot_tb(both, w_in).astype(bf16)
            return dot_ta(x, both), dot_ta(mid, r)

        a_gu, a_d = part(0)
        b_gu, b_d = part(TILE)
        gu = a_gu + b_gu
        ogu[slot, 0] = gu[:, :ff]
        ogu[slot, 1] = gu[:, ff:]
        od[slot] = a_d + b_d
        for first in range(2 * TILE, plan.rows, TILE):
            @pl.when(exp_wins[exp] * WIN > first)
            def _(first=first):
                c_gu, c_d = part(first)
                ogu[slot, 0] += c_gu[:, :ff]
                ogu[slot, 1] += c_gu[:, ff:]
                od[slot] += c_d

        for store in stores(exp, slot):
            store.start()
        return 0

    lax.fori_loop(0, plan.experts, expert, 0)
    for exp in (plan.experts - 2, plan.experts - 1):
        for store in stores(exp, exp % 2):
            store.wait()

    def combine(tile, _):
        combine_tile(plan, tab, win_dst, win_chunks, lr, gt, tile, buf, y, False)
        return 0

    half = plan.tiles // 2
    lax.fori_loop(half, plan.tiles, combine, 0)
    far = pltpu.make_async_copy(y.at[pl.ds(2 * n_tok, 2 * n_tok)], y_far, sems.at[0])
    far.start()
    lax.fori_loop(0, half, combine, 0)
    near = pltpu.make_async_copy(y.at[pl.ds(0, 2 * n_tok)], y_near, sems.at[1])
    near.start()
    far.wait()
    near.wait()


SMEM = pl.BlockSpec(memory_space=pltpu.SMEM)
VMEM = pl.BlockSpec(memory_space=pltpu.VMEM)
ANY = pl.BlockSpec(memory_space=pl.ANY)
LIMIT = 60 * 1024 * 1024


def weight_scratch(plan):
    e, d, f = plan.experts, plan.width, plan.ff
    return [pltpu.VMEM((e, d, f), bf16), pltpu.VMEM((e, d, f), bf16), pltpu.VMEM((e, f, d), bf16)]


def run_forward(plan, tables, z, weights):
    flops = 2 * plan.buf_rows * plan.width * plan.width * 4
    half = jax.ShapeDtypeStruct((plan.total // 2, plan.width), f32)
    return pl.pallas_call(
        functools.partial(forward_kernel, plan),
        out_shape=(half, half),
        in_specs=[SMEM] * 5 + [VMEM] * 2 + [ANY] * 6,
        out_specs=(ANY, ANY),
        scratch_shapes=[pltpu.VMEM((plan.total, plan.width), bf16)] + weight_scratch(plan) + [
            pltpu.VMEM((plan.buf_rows, plan.width), bf16),
            pltpu.VMEM((plan.total, plan.width), f32),
            pltpu.SemaphoreType.DMA((6,)),
        ],
        compiler_params=pltpu.CompilerParams(vmem_limit_bytes=LIMIT),
        cost_estimate=pl.CostEstimate(flops=flops, bytes_accessed=0, transcendentals=0),
        name="expert_forward",
    )(*tables, *z, *weights)


def run_backward(plan, tables, z, g, weights):
    e, d, f = plan.experts, plan.width, plan.ff
    flops = 2 * plan.buf_rows * plan.width * plan.width * 8
    half = jax.ShapeDtypeStruct((plan.total // 2, plan.width), f32)
    return pl.pallas_call(
        functools.partial(backward_kernel, plan),
        out_shape=(half, half, jax.ShapeDtypeStruct((e, d, f), f32), jax.ShapeDtypeStruct((e, d, f), f32), jax.ShapeDtypeStruct((e, f, d), f32)),
        in_specs=[SMEM] * 5 + [VMEM] * 2 + [ANY] * 9,
        out_specs=(ANY,) * 5,
        scratch_shapes=[pltpu.VMEM((2, plan.total, plan.width), bf16)] + weight_scratch(plan) + [
            pltpu.VMEM((plan.buf_rows, plan.width), bf16),
            pltpu.VMEM((plan.buf_rows, plan.width), bf16),
            pltpu.VMEM((plan.total, plan.width), f32),
            pltpu.VMEM((2, 2, d, f), f32),
            pltpu.VMEM((2, f, d), f32),
            pltpu.SemaphoreType.DMA((9,)),
            pltpu.SemaphoreType.DMA((2, 3)),
        ],
        compiler_params=pltpu.CompilerParams(vmem_limit_bytes=LIMIT),
        cost_estimate=pl.CostEstimate(flops=flops, bytes_accessed=0, transcendentals=0),
        name="expert_backward",
    )(*tables, *z, *g, *weights)


def solution(mesh):
    groups = mesh.shape['ep']
    stages = mesh.shape['pp']
    to_next = [(sender, (sender + 1) % stages) for sender in range(stages)]
    to_prev = [(sender, (sender - 1) % stages) for sender in range(stages)]
    core_pairs = [(dev, dev ^ 1) for dev in range(groups)]
    chip_pairs = [(dev, dev ^ 2) for dev in range(groups)]

    def swap_core(value):
        return lax.ppermute(value, 'ep', core_pairs)

    def swap_chip(value):
        return lax.ppermute(value, 'ep', chip_pairs)

    def local_step(x_fwd, x_bwd, grad_in, dense_in, dense_out, exp_gate, exp_up, exp_down, route_fwd, gate_fwd, route_bwd, gate_bwd):
        n_tok, width = x_fwd.shape[1], x_fwd.shape[2]
        choices = route_fwd.shape[3]
        experts, ff = exp_gate.shape[2], exp_gate.shape[4]
        plan = Plan(n_tok, groups, experts, choices, width, ff)
        capacity = 2 * n_tok * choices // (experts * groups)
        me = lax.axis_index('ep')

        def gather_rows(rows):
            far = swap_chip(rows)
            return rows, far, swap_core(jnp.concatenate([rows, far], 0))

        def scatter_sum(near, far):
            pair = near + swap_core(far)
            return pair[:n_tok] + swap_chip(pair[n_tok:])

        routes = jnp.concatenate([route_fwd[0], route_bwd[0]], 0)
        gates = jnp.concatenate([gate_fwd[0], gate_bwd[0]], 0)
        packed = jnp.stack([(routes // capacity).astype(bf16), gates]).transpose(0, 1, 3, 2)
        far = swap_chip(packed)
        mine = jnp.concatenate([packed, far], -1)
        whole = jnp.concatenate([mine, swap_core(mine)], -1)
        picks = whole[0].astype(jnp.int32) - me * experts
        gate_all = whole[1].astype(f32)
        match = picks[:, :, None, :] == jnp.arange(experts, dtype=jnp.int32)[None, None, :, None]
        chosen = jnp.sum(match.astype(f32), 1)
        gate_of = jnp.sum(jnp.where(match, gate_all[:, :, None, :], 0.0), 1)
        tiled = chosen.reshape(4, experts, plan.tiles, TILE)
        before = (jnp.arange(TILE)[:, None] < jnp.arange(TILE)[None, :]).astype(bf16)
        rank = jnp.einsum('qejt,ts->qejs', tiled.astype(bf16), before, preferred_element_type=f32)
        local_rank = jnp.where(tiled > 0, rank, -1.0).astype(jnp.int32).reshape(4, experts, plan.total)
        count = jnp.sum(tiled, -1).astype(jnp.int32)
        wins = (count + (WIN - 1)) // WIN
        in_tile = jnp.cumsum(wins, 1) - wins
        in_exp = jnp.cumsum(wins, 2) - wins
        tile_wins = jnp.sum(wins, 1)
        exp_wins = jnp.sum(wins, 2)
        spots = jnp.arange(plan.per_tile, dtype=jnp.int32)[None, None, :, None]
        start = in_tile.transpose(0, 2, 1)[:, :, None, :]
        size = wins.transpose(0, 2, 1)[:, :, None, :]
        owner = (spots >= start) & (spots < start + size)
        ids = jnp.arange(experts, dtype=jnp.int32)
        shift = (ids[None, :, None] * plan.per_exp + in_exp - in_tile).transpose(0, 2, 1)[:, :, None, :]
        used = jnp.any(owner, -1)
        win_exp = jnp.sum(jnp.where(owner, ids, 0), -1)
        win_base = jnp.where(used, jnp.sum(jnp.where(owner, (spots - start) * WIN, 0), -1), 1 << 20)
        win_dst = jnp.where(used, jnp.sum(jnp.where(owner, spots + shift, 0), -1), plan.trash)
        win_chunks = (tile_wins + (CHUNK - 1)) // CHUNK

        def tables(which):
            return (win_exp[which].reshape(-1), win_base[which].reshape(-1), win_dst[which].reshape(-1), win_chunks[which], exp_wins[which], local_rank[which], gate_of[which])

        def front(tokens, block):
            pre_act, hidden = dense_forward(tokens, dense_in[0, block], dense_out[0, block])
            normed = rms_norm(hidden.astype(f32)).astype(bf16)
            return pre_act, hidden, gather_rows(normed)

        def exp_weights(block):
            return exp_gate[0, block], exp_up[0, block], exp_down[0, block]

        def finish(hidden, rows, which, block):
            mixed = scatter_sum(*run_forward(plan, tables(which), rows, exp_weights(block)))
            return (hidden.astype(f32) + mixed).astype(bf16)

        def backward(grad_out, grad_rows, tokens, saved, which, block):
            pre_act, hidden, rows = saved
            near, far, dwg, dwu, dwd = run_backward(plan, tables(which), rows, grad_rows, exp_weights(block))
            grad_norm = scatter_sum(near, far)
            grad_hidden = grad_out.astype(f32) + rms_back(hidden.astype(f32), grad_norm)
            return dense_backward(grad_hidden, tokens, pre_act, dense_in[0, block], dense_out[0, block]), dwg, dwu, dwd

        tok_b = x_bwd[0]
        saved_one = front(tok_b, 0)
        tok_f = x_fwd[0]
        _, hid_f, rows_f = front(tok_f, 0)
        grads_two = gather_rows(grad_in[0])
        mid_b = finish(saved_one[1], saved_one[2], 2, 0)
        saved_two = front(mid_b, 1)
        mid_f = finish(hid_f, rows_f, 0, 0)
        _, hid_g, rows_g = front(mid_f, 1)
        grad_mid, wg_two, wu_two, wd_two = backward(grad_in[0], grads_two, mid_b, saved_two, 3, 1)
        out_f = finish(hid_g, rows_g, 1, 1)
        grad_first, wg_one, wu_one, wd_one = backward(grad_mid, gather_rows(grad_mid), tok_b, saved_one, 2, 0)
        y_next = lax.ppermute(out_f, 'pp', to_next)
        dx_prev = lax.ppermute(grad_first, 'pp', to_prev)
        return (y_next[None], dx_prev[None], jnp.stack([wg_one, wg_two])[None], jnp.stack([wu_one, wu_two])[None], jnp.stack([wd_one, wd_two])[None])

    tok_spec = P('pp', 'ep', None)
    dense_spec = P('pp', None, None, None)
    exp_spec = P('pp', None, 'ep', None, None)
    route_spec = P('pp', None, 'ep', None)
    return jax.shard_map(local_step, mesh=mesh, in_specs=(tok_spec, tok_spec, tok_spec, dense_spec, dense_spec, exp_spec, exp_spec, exp_spec, route_spec, route_spec, route_spec, route_spec), out_specs=(tok_spec, tok_spec, exp_spec, exp_spec, exp_spec), check_vma=False)
```

```python
import functools

import jax
import jax.numpy as jnp
from jax import lax
from jax.experimental import pallas as pl
from jax.experimental.pallas import tpu as pltpu
from jax.sharding import PartitionSpec as P

NORM_EPS = 1e-6
WIN = 16
TILE = 256
CHUNK = 16
MAIN = 4

f32 = jnp.float32
bf16 = jnp.bfloat16


def rms_norm(values):
    return values * lax.rsqrt(jnp.mean(values * values, axis=-1, keepdims=True) + NORM_EPS)


def rms_back(values, grad_out):
    inv_rms = lax.rsqrt(jnp.mean(values * values, axis=-1, keepdims=True) + NORM_EPS)
    proj_mean = jnp.mean(grad_out * values, axis=-1, keepdims=True)
    return inv_rms * grad_out - values * (inv_rms * inv_rms * inv_rms) * proj_mean


def silu_grad(pre_act):
    sig_value = jax.nn.sigmoid(pre_act)
    return sig_value * (1.0 + pre_act * (1.0 - sig_value))


def dense_forward(tokens, w_in, w_out):
    normed = rms_norm(tokens.astype(f32)).astype(bf16)
    pre_act = jnp.dot(normed, w_in, preferred_element_type=f32)
    mid_act = jax.nn.silu(pre_act).astype(bf16)
    hidden = (tokens.astype(f32) + jnp.dot(mid_act, w_out, preferred_element_type=f32)).astype(bf16)
    return pre_act, hidden


def dense_backward(grad_hidden, tokens, pre_act, w_in, w_out):
    grad_dense = jnp.einsum('td,fd->tf', grad_hidden.astype(bf16), w_out, preferred_element_type=f32)
    grad_pre = (grad_dense * silu_grad(pre_act)).astype(bf16)
    grad_act = jnp.einsum('tf,df->td', grad_pre, w_in, preferred_element_type=f32)
    return (grad_hidden + rms_back(tokens.astype(f32), grad_act)).astype(bf16)


class Plan:
    def __init__(self, n_tok, groups, experts, choices, width, ff):
        self.n_tok, self.groups, self.experts, self.width, self.ff = n_tok, groups, experts, width, ff
        self.total = n_tok * groups
        self.tiles = self.total // TILE
        capacity = 2 * n_tok * choices // (experts * groups)
        worst = (TILE * choices + experts * (WIN - 1)) // WIN
        self.per_tile = -(-worst // CHUNK) * CHUNK
        self.per_exp = -(-(groups * capacity + self.tiles * (WIN - 1)) // (WIN * 16)) * 16
        self.rows = self.per_exp * WIN
        self.trash = experts * self.per_exp
        self.buf_rows = (self.trash + 1) * WIN


def one_hot_rows(plan, tab, lr, gt, tile, chunk, plain, gated):
    win_exp, win_base = tab
    lane = pl.ds(pl.multiple_of(tile * TILE, TILE), TILE)
    iota = lax.broadcasted_iota(jnp.int32, (WIN, TILE), 0)
    ones, gates = [], []
    for i in range(CHUNK):
        spot = tile * plan.per_tile + chunk * CHUNK + i
        exp = win_exp[spot]
        hit = (lr[pl.ds(exp, 1), lane] - win_base[spot]) == iota
        if plain:
            ones.append(jnp.where(hit, 1.0, 0.0).astype(bf16))
        if gated:
            gates.append(jnp.where(hit, gt[pl.ds(exp, 1), lane], 0.0).astype(bf16))
    return (jnp.concatenate(ones, 0) if plain else None), (jnp.concatenate(gates, 0) if gated else None)


def win_rows(plan, win_dst, tile, chunk, i):
    dst = win_dst[tile * plan.per_tile + chunk * CHUNK + i]
    return pl.ds(pl.multiple_of(dst * WIN, WIN), WIN)


def dot(a, b):
    return jnp.dot(a, b, preferred_element_type=f32)


def dot_tb(a, b):
    return lax.dot_general(a, b, (((1,), (1,)), ((), ())), preferred_element_type=f32)


def dot_ta(a, b):
    return lax.dot_general(a, b, (((0,), (0,)), ((), ())), preferred_element_type=f32)


def combine_tile(plan, tab, win_dst, win_chunks, lr, gt, tile, buf, out, gated):
    def piece(chunk):
        ones, gates = one_hot_rows(plan, tab, lr, gt, tile, chunk, not gated, gated)
        rows = jnp.concatenate([buf[win_rows(plan, win_dst, tile, chunk, i), :] for i in range(CHUNK)], 0)
        return dot_ta(gates if gated else ones, rows)

    total = piece(0)
    for chunk in range(1, MAIN):
        total = total + piece(chunk)
    span = pl.ds(pl.multiple_of(tile * TILE, TILE), TILE)
    out[span, :] = total

    def more(chunk, _):
        out[span, :] += piece(chunk)
        return 0

    lax.fori_loop(MAIN, jnp.maximum(win_chunks[tile], MAIN), more, 0)


def load_pieces(pieces, whole, sems, first):
    n_tok = pieces[0].shape[0]
    return [pltpu.make_async_copy(src, whole.at[pl.ds(i * n_tok, n_tok)], sems.at[first + i]) for i, src in enumerate(pieces)]


def load_weights(block, sources, targets, sems, first):
    return [pltpu.make_async_copy(src.at[0, block], dst, sems.at[first + i]) for i, (src, dst) in enumerate(zip(sources, targets))]


def chunks_of(win_chunks, tile, piece):
    for chunk in range(MAIN):
        piece(chunk)

    def more(chunk, _):
        piece(chunk)
        return 0

    lax.fori_loop(MAIN, jnp.maximum(win_chunks[tile], MAIN), more, 0)


def combine_all(plan, combine, y, outs, sems):
    n_tok = plan.n_tok
    per = n_tok // TILE
    sends = [pltpu.make_async_copy(y.at[pl.ds(piece * n_tok, n_tok)], outs[piece], sems.at[piece]) for piece in range(4)]

    def step(i, _):
        tile = plan.tiles - 1 - i
        combine(tile, 0)
        for piece in range(4):
            pl.when(tile == piece * per)(sends[piece].start)
        return 0

    lax.fori_loop(0, plan.tiles, step, 0)
    for send in sends:
        send.wait()


def forward_kernel(plan, block, win_exp, win_base, win_dst, win_chunks, exp_wins, lr, gt, z0, z1, z2, z3, wg_in, wu_in, wd_in, y0, y1, y2, y3, z, wg, wu, wd, buf, y, mid_a, mid_b, sems):
    ff = plan.ff
    loads = load_pieces((z0, z1, z2, z3), z, sems, 0)
    weights = load_weights(block, (wg_in, wu_in, wd_in), (wg, wu, wd), sems, 4)
    for load in loads + weights:
        load.start()
    tab = (win_exp, win_base)
    for load in loads:
        load.wait()

    def dispatch(tile, _):
        rows = z[pl.ds(pl.multiple_of(tile * TILE, TILE), TILE), :]

        def piece(chunk):
            ones, _ = one_hot_rows(plan, tab, lr, gt, tile, chunk, True, False)
            moved = dot(ones, rows).astype(bf16)
            for i in range(CHUNK):
                buf[win_rows(plan, win_dst, tile, chunk, i), :] = moved[i * WIN:(i + 1) * WIN, :]

        chunks_of(win_chunks, tile, piece)
        return 0

    lax.fori_loop(0, plan.tiles, dispatch, 0)
    for load in weights:
        load.wait()

    def span_of(exp, first):
        return pl.ds(pl.multiple_of(exp * plan.rows + first, TILE), TILE)

    def middle(exp, span):
        pre = dot(buf[span, :], jnp.concatenate([wg[exp], wu[exp]], 1))
        return (jax.nn.silu(pre[:, :ff]) * pre[:, ff:]).astype(bf16)

    def first_half(exp, mid):
        for i in range(2):
            mid[i * TILE:(i + 1) * TILE, :] = middle(exp, span_of(exp, i * TILE))

    def second_half(exp, mid):
        for i in range(2):
            buf[span_of(exp, i * TILE), :] = dot(mid[i * TILE:(i + 1) * TILE, :], wd[exp]).astype(bf16)

    def pair(step, _):
        exp = 2 * step
        first_half(exp + 1, mid_b)
        second_half(exp, mid_a)
        first_half(jnp.minimum(exp + 2, plan.experts - 1), mid_a)
        second_half(exp + 1, mid_b)
        return 0

    first_half(0, mid_a)
    lax.fori_loop(0, plan.experts // 2, pair, 0)

    def rest(exp, _):
        for first in range(2 * TILE, plan.rows, TILE):
            @pl.when(exp_wins[exp] * WIN > first)
            def _(first=first):
                span = span_of(exp, first)
                buf[span, :] = dot(middle(exp, span), wd[exp]).astype(bf16)
        return 0

    lax.fori_loop(0, plan.experts, rest, 0)

    def combine(tile, _):
        combine_tile(plan, tab, win_dst, win_chunks, lr, gt, tile, buf, y, True)
        return 0

    combine_all(plan, combine, y, (y0, y1, y2, y3), sems)


def backward_kernel(plan, block, aliased, *refs):
    win_exp, win_base, win_dst, win_chunks, exp_wins, lr, gt = refs[:7]
    z_in, g_in, w_src = refs[7:11], refs[11:15], refs[15:18]
    refs = refs[21:] if aliased else refs[18:]
    outs, (dwg, dwu, dwd) = refs[:4], refs[4:7]
    z, g, wg, wu, wd, buf, rbuf, y, mid_a, mid_b, both_a, both_b, og, ou, od, sems, osems = refs[7:]
    width, ff = plan.width, plan.ff
    loads = load_pieces(z_in, z, sems, 0) + load_pieces(g_in, g, sems, 4)
    weights = load_weights(block, w_src, (wg, wu, wd), sems, 8)
    for load in loads + weights:
        load.start()
    tab = (win_exp, win_base)

    def clear(step, _):
        span = pl.ds(pl.multiple_of(step * TILE, TILE), TILE)
        buf[span, :] = jnp.zeros((TILE, width), bf16)
        rbuf[span, :] = jnp.zeros((TILE, width), bf16)
        return 0

    lax.fori_loop(0, plan.experts * plan.rows // TILE, clear, 0)
    for load in loads:
        load.wait()

    def dispatch(tile, _):
        span = pl.ds(pl.multiple_of(tile * TILE, TILE), TILE)
        z_rows, g_rows = z[span, :], g[span, :]

        def piece(chunk):
            ones, gates = one_hot_rows(plan, tab, lr, gt, tile, chunk, True, True)
            moved = dot(ones, z_rows).astype(bf16)
            sent = dot(gates, g_rows).astype(bf16)
            for i in range(CHUNK):
                dst = win_rows(plan, win_dst, tile, chunk, i)
                buf[dst, :] = moved[i * WIN:(i + 1) * WIN, :]
                rbuf[dst, :] = sent[i * WIN:(i + 1) * WIN, :]

        chunks_of(win_chunks, tile, piece)
        return 0

    lax.fori_loop(0, plan.tiles, dispatch, 0)
    for load in weights:
        load.wait()

    def span_of(exp, first):
        return pl.ds(pl.multiple_of(exp * plan.rows + first, TILE), TILE)

    def stores(exp, slot):
        return [pltpu.make_async_copy(src.at[slot], dst.at[block, exp], osems.at[slot, i]) for i, (src, dst) in enumerate(((og, dwg), (ou, dwu), (od, dwd)))]

    def in_weights(exp):
        return jnp.concatenate([wg[exp], wu[exp]], 1)

    def first_part(exp, first, mid, both, row):
        span = span_of(exp, first)
        pre = dot(buf[span, :], in_weights(exp))
        grad_mid = dot_tb(rbuf[span, :], wd[exp])
        gate_pre, up_pre = pre[:, :ff], pre[:, ff:]
        sig = jax.nn.sigmoid(gate_pre)
        act = gate_pre * sig
        mid[row:row + TILE, :] = (act * up_pre).astype(bf16)
        both[row:row + TILE, :ff] = (grad_mid * up_pre * (sig * (1.0 + gate_pre * (1.0 - sig)))).astype(bf16)
        both[row:row + TILE, ff:] = (grad_mid * act).astype(bf16)

    def second_part(exp, first, count, mid, both):
        spans = pl.ds(pl.multiple_of(exp * plan.rows + first, TILE), count)
        gu = dot_ta(buf[spans, :], both[0:count, :])
        down = dot_ta(mid[0:count, :], rbuf[spans, :])
        buf[spans, :] = dot_tb(both[0:count, :], in_weights(exp)).astype(bf16)
        return gu, down

    def first_half(exp, mid, both):
        for i in range(2):
            first_part(exp, i * TILE, mid, both, i * TILE)

    def second_half(exp, mid, both, slot, wait):
        @pl.when(wait)
        def _():
            for store in stores(exp, slot):
                store.wait()

        gu, down = second_part(exp, 0, 2 * TILE, mid, both)
        og[slot] = gu[:, :ff]
        ou[slot] = gu[:, ff:]
        od[slot] = down

    def send(exp, mid, both, slot):
        for first in range(2 * TILE, plan.rows, TILE):
            @pl.when(exp_wins[exp] * WIN > first)
            def _(first=first):
                first_part(exp, first, mid, both, 0)
                gu, down = second_part(exp, first, TILE, mid, both)
                og[slot] += gu[:, :ff]
                ou[slot] += gu[:, ff:]
                od[slot] += down

        for store in stores(exp, slot):
            store.start()

    def pair(step, _):
        exp = 2 * step
        first_half(exp + 1, mid_b, both_b)
        second_half(exp, mid_a, both_a, 0, step > 0)
        send(exp, mid_a, both_a, 0)
        first_half(jnp.minimum(exp + 2, plan.experts - 1), mid_a, both_a)
        second_half(exp + 1, mid_b, both_b, 1, step > 0)
        send(exp + 1, mid_b, both_b, 1)
        return 0

    first_half(0, mid_a, both_a)
    lax.fori_loop(0, plan.experts // 2, pair, 0)
    for slot in range(2):
        for store in stores(plan.experts - 2 + slot, slot):
            store.wait()

    def combine(tile, _):
        combine_tile(plan, tab, win_dst, win_chunks, lr, gt, tile, buf, y, False)
        return 0

    combine_all(plan, combine, y, outs, sems)


SMEM = pl.BlockSpec(memory_space=pltpu.SMEM)
VMEM = pl.BlockSpec(memory_space=pltpu.VMEM)
ANY = pl.BlockSpec(memory_space=pl.ANY)
LIMIT = 60 * 1024 * 1024


def weight_scratch(plan):
    e, d, f = plan.experts, plan.width, plan.ff
    return [pltpu.VMEM((e, d, f), bf16), pltpu.VMEM((e, d, f), bf16), pltpu.VMEM((e, f, d), bf16)]


def run_forward(plan, block, tables, z, weights):
    flops = 2 * plan.buf_rows * plan.width * plan.width * 4
    piece = jax.ShapeDtypeStruct((plan.n_tok, plan.width), f32)
    return pl.pallas_call(
        functools.partial(forward_kernel, plan, block),
        out_shape=(piece,) * 4,
        in_specs=[SMEM] * 5 + [VMEM] * 2 + [ANY] * 7,
        out_specs=(ANY,) * 4,
        scratch_shapes=[pltpu.VMEM((plan.total, plan.width), bf16)] + weight_scratch(plan) + [
            pltpu.VMEM((plan.buf_rows, plan.width), bf16),
            pltpu.VMEM((plan.total, plan.width), f32),
            pltpu.VMEM((2 * TILE, plan.ff), bf16),
            pltpu.VMEM((2 * TILE, plan.ff), bf16),
            pltpu.SemaphoreType.DMA((7,)),
        ],
        compiler_params=pltpu.CompilerParams(vmem_limit_bytes=LIMIT),
        cost_estimate=pl.CostEstimate(flops=flops, bytes_accessed=0, transcendentals=0),
        name="expert_forward",
    )(*tables, *z, *weights)


def run_backward(plan, block, tables, z, g, weights, grads):
    e, d, f = plan.experts, plan.width, plan.ff
    flops = 2 * plan.buf_rows * plan.width * plan.width * 8
    piece = jax.ShapeDtypeStruct((plan.n_tok, plan.width), f32)
    up = jax.ShapeDtypeStruct((2, e, d, f), f32)
    down = jax.ShapeDtypeStruct((2, e, f, d), f32)
    return pl.pallas_call(
        functools.partial(backward_kernel, plan, block, bool(grads)),
        out_shape=(piece,) * 4 + (up, up, down),
        in_specs=[SMEM] * 5 + [VMEM] * 2 + [ANY] * (11 + len(grads)),
        out_specs=(ANY,) * 7,
        scratch_shapes=[pltpu.VMEM((plan.total, plan.width), bf16)] * 2 + weight_scratch(plan) + [
            pltpu.VMEM((plan.buf_rows, plan.width), bf16),
            pltpu.VMEM((plan.buf_rows, plan.width), bf16),
            pltpu.VMEM((plan.total, plan.width), f32),
            pltpu.VMEM((2 * TILE, f), bf16),
            pltpu.VMEM((2 * TILE, f), bf16),
            pltpu.VMEM((2 * TILE, 2 * f), bf16),
            pltpu.VMEM((2 * TILE, 2 * f), bf16),
            pltpu.VMEM((2, d, f), f32),
            pltpu.VMEM((2, d, f), f32),
            pltpu.VMEM((2, f, d), f32),
            pltpu.SemaphoreType.DMA((11,)),
            pltpu.SemaphoreType.DMA((2, 3)),
        ],
        input_output_aliases={18 + i: 4 + i for i in range(len(grads))},
        compiler_params=pltpu.CompilerParams(vmem_limit_bytes=LIMIT),
        cost_estimate=pl.CostEstimate(flops=flops, bytes_accessed=0, transcendentals=0),
        name="expert_backward",
    )(*tables, *z, *g, *weights, *grads)


def solution(mesh):
    groups = mesh.shape['ep']
    stages = mesh.shape['pp']
    to_next = [(sender, (sender + 1) % stages) for sender in range(stages)]
    to_prev = [(sender, (sender - 1) % stages) for sender in range(stages)]
    core_pairs = [(dev, dev ^ 1) for dev in range(groups)]
    chip_pairs = [(dev, dev ^ 2) for dev in range(groups)]

    def swap_core(value):
        return lax.ppermute(value, 'ep', core_pairs)

    def swap_chip(value):
        return lax.ppermute(value, 'ep', chip_pairs)

    def local_step(x_fwd, x_bwd, grad_in, dense_in, dense_out, exp_gate, exp_up, exp_down, route_fwd, gate_fwd, route_bwd, gate_bwd):
        n_tok, width = x_fwd.shape[1], x_fwd.shape[2]
        choices = route_fwd.shape[3]
        experts, ff = exp_gate.shape[2], exp_gate.shape[4]
        plan = Plan(n_tok, groups, experts, choices, width, ff)
        capacity = 2 * n_tok * choices // (experts * groups)
        me = lax.axis_index('ep')

        def gather_rows(rows):
            far = swap_chip(rows)
            return rows, far, swap_core(rows), swap_core(far)

        def scatter_sum(y0, y1, y2, y3):
            far = swap_chip(y1 + swap_core(y3))
            return y0 + swap_core(y2) + far

        routes = jnp.concatenate([route_fwd[0], route_bwd[0]], 0)
        gates = jnp.concatenate([gate_fwd[0], gate_bwd[0]], 0)
        packed = jnp.stack([(routes // capacity).astype(bf16), gates]).transpose(0, 1, 3, 2)
        far = swap_chip(packed)
        mine = jnp.concatenate([packed, far], -1)
        whole = jnp.concatenate([mine, swap_core(mine)], -1)
        picks = whole[0].astype(jnp.int32) - me * experts
        gate_all = whole[1].astype(f32)
        match = picks[:, :, None, :] == jnp.arange(experts, dtype=jnp.int32)[None, None, :, None]
        chosen = jnp.sum(match.astype(f32), 1)
        gate_of = jnp.sum(jnp.where(match, gate_all[:, :, None, :], 0.0), 1)
        tiled = chosen.reshape(4, experts, plan.tiles, TILE)
        before = (jnp.arange(TILE)[:, None] < jnp.arange(TILE)[None, :]).astype(bf16)
        rank = jnp.einsum('qejt,ts->qejs', tiled.astype(bf16), before, preferred_element_type=f32)
        local_rank = jnp.where(tiled > 0, rank, -1.0).astype(jnp.int32).reshape(4, experts, plan.total)
        count = jnp.sum(tiled, -1).astype(jnp.int32)
        wins = (count + (WIN - 1)) // WIN
        in_tile = jnp.cumsum(wins, 1) - wins
        in_exp = jnp.cumsum(wins, 2) - wins
        tile_wins = jnp.sum(wins, 1)
        exp_wins = jnp.sum(wins, 2)
        spots = jnp.arange(plan.per_tile, dtype=jnp.int32)[None, None, :, None]
        start = in_tile.transpose(0, 2, 1)[:, :, None, :]
        size = wins.transpose(0, 2, 1)[:, :, None, :]
        owner = (spots >= start) & (spots < start + size)
        ids = jnp.arange(experts, dtype=jnp.int32)
        shift = (ids[None, :, None] * plan.per_exp + in_exp - in_tile).transpose(0, 2, 1)[:, :, None, :]
        used = jnp.any(owner, -1)
        win_exp = jnp.sum(jnp.where(owner, ids, 0), -1)
        win_base = jnp.where(used, jnp.sum(jnp.where(owner, (spots - start) * WIN, 0), -1), 1 << 20)
        win_dst = jnp.where(used, jnp.sum(jnp.where(owner, spots + shift, 0), -1), plan.trash)
        win_chunks = (tile_wins + (CHUNK - 1)) // CHUNK

        def tables(which):
            return (win_exp[which].reshape(-1), win_base[which].reshape(-1), win_dst[which].reshape(-1), win_chunks[which], exp_wins[which], local_rank[which], gate_of[which])

        def front(tokens, block):
            pre_act, hidden = dense_forward(tokens, dense_in[0, block], dense_out[0, block])
            normed = rms_norm(hidden.astype(f32)).astype(bf16)
            return pre_act, hidden, gather_rows(normed)

        weights = (exp_gate, exp_up, exp_down)

        def finish(hidden, rows, which, block):
            mixed = scatter_sum(*run_forward(plan, block, tables(which), rows, weights))
            return (hidden.astype(f32) + mixed).astype(bf16)

        def backward(grad_out, grad_rows, tokens, saved, which, block, grads):
            pre_act, hidden, rows = saved
            results = run_backward(plan, block, tables(which), rows, grad_rows, weights, grads)
            grad_norm = scatter_sum(*results[:4])
            grad_hidden = grad_out.astype(f32) + rms_back(hidden.astype(f32), grad_norm)
            return dense_backward(grad_hidden, tokens, pre_act, dense_in[0, block], dense_out[0, block]), results[4:]

        tok_b = x_bwd[0]
        saved_one = front(tok_b, 0)
        tok_f = x_fwd[0]
        _, hid_f, rows_f = front(tok_f, 0)
        grads_two = gather_rows(grad_in[0])
        mid_b = finish(saved_one[1], saved_one[2], 2, 0)
        saved_two = front(mid_b, 1)
        mid_f = finish(hid_f, rows_f, 0, 0)
        _, hid_g, rows_g = front(mid_f, 1)
        grad_mid, sums = backward(grad_in[0], grads_two, mid_b, saved_two, 3, 1, ())
        out_f = finish(hid_g, rows_g, 1, 1)
        grad_first, sums = backward(grad_mid, gather_rows(grad_mid), tok_b, saved_one, 2, 0, sums)
        y_next = lax.ppermute(out_f, 'pp', to_next)
        dx_prev = lax.ppermute(grad_first, 'pp', to_prev)
        return (y_next[None], dx_prev[None], sums[0][None], sums[1][None], sums[2][None])

    tok_spec = P('pp', 'ep', None)
    dense_spec = P('pp', None, None, None)
    exp_spec = P('pp', None, 'ep', None, None)
    route_spec = P('pp', None, 'ep', None)
    return jax.shard_map(local_step, mesh=mesh, in_specs=(tok_spec, tok_spec, tok_spec, dense_spec, dense_spec, exp_spec, exp_spec, exp_spec, route_spec, route_spec, route_spec, route_spec), out_specs=(tok_spec, tok_spec, exp_spec, exp_spec, exp_spec), check_vma=False)
```

```python
import functools

import jax
import jax.numpy as jnp
from jax import lax
from jax.experimental import pallas as pl
from jax.experimental.pallas import tpu as pltpu
from jax.sharding import PartitionSpec as P


NORM_EPS = 1e-6
WIN = 16
TILE = 256
CHUNK = 16
MAIN = 4

f32 = jnp.float32
bf16 = jnp.bfloat16


def rms_norm(values):
    return values * lax.rsqrt(jnp.mean(values * values, axis=-1, keepdims=True) + NORM_EPS)


def rms_back(values, grad_out):
    inv_rms = lax.rsqrt(jnp.mean(values * values, axis=-1, keepdims=True) + NORM_EPS)
    proj_mean = jnp.mean(grad_out * values, axis=-1, keepdims=True)
    return inv_rms * grad_out - values * (inv_rms * inv_rms * inv_rms) * proj_mean


def silu_grad(pre_act):
    sig_value = jax.nn.sigmoid(pre_act)
    return sig_value * (1.0 + pre_act * (1.0 - sig_value))


def dense_forward(tokens, w_in, w_out):
    normed = rms_norm(tokens.astype(f32)).astype(bf16)
    pre_act = jnp.dot(normed, w_in, preferred_element_type=f32)
    mid_act = jax.nn.silu(pre_act).astype(bf16)
    hidden = (tokens.astype(f32) + jnp.dot(mid_act, w_out, preferred_element_type=f32)).astype(bf16)
    return pre_act, hidden


def dense_backward(grad_hidden, tokens, pre_act, w_in, w_out):
    grad_dense = jnp.einsum('td,fd->tf', grad_hidden.astype(bf16), w_out, preferred_element_type=f32)
    grad_pre = (grad_dense * silu_grad(pre_act)).astype(bf16)
    grad_act = jnp.einsum('tf,df->td', grad_pre, w_in, preferred_element_type=f32)
    return (grad_hidden + rms_back(tokens.astype(f32), grad_act)).astype(bf16)


class Plan:
    def __init__(self, n_tok, groups, experts, choices, width, ff):
        self.n_tok, self.groups, self.experts, self.width, self.ff = n_tok, groups, experts, width, ff
        self.total = n_tok * groups
        self.tiles = self.total // TILE
        capacity = 2 * n_tok * choices // (experts * groups)
        worst = (TILE * choices + experts * (WIN - 1)) // WIN
        self.per_tile = -(-worst // CHUNK) * CHUNK
        self.per_exp = -(-(groups * capacity + self.tiles * (WIN - 1)) // (WIN * 16)) * 16
        self.rows = self.per_exp * WIN
        self.trash = experts * self.per_exp
        self.buf_rows = (self.trash + 1) * WIN


def one_hot_rows(plan, tab, lr, gt, tile, chunk, plain, gated):
    win_exp, win_base = tab
    lane = pl.ds(pl.multiple_of(tile * TILE, TILE), TILE)
    iota = lax.broadcasted_iota(jnp.int32, (WIN, TILE), 0)
    ones, gates = [], []
    for i in range(CHUNK):
        spot = tile * plan.per_tile + chunk * CHUNK + i
        exp = win_exp[spot]
        hit = (lr[pl.ds(exp, 1), lane] - win_base[spot]) == iota
        if plain:
            ones.append(jnp.where(hit, 1.0, 0.0).astype(bf16))
        if gated:
            gates.append(jnp.where(hit, gt[pl.ds(exp, 1), lane], 0.0).astype(bf16))
    return (jnp.concatenate(ones, 0) if plain else None), (jnp.concatenate(gates, 0) if gated else None)


def win_rows(plan, win_dst, tile, chunk, i):
    dst = win_dst[tile * plan.per_tile + chunk * CHUNK + i]
    return pl.ds(pl.multiple_of(dst * WIN, WIN), WIN)


def dot(a, b):
    return jnp.dot(a, b, preferred_element_type=f32)


def dot_tb(a, b):
    return lax.dot_general(a, b, (((1,), (1,)), ((), ())), preferred_element_type=f32)


def dot_ta(a, b):
    return lax.dot_general(a, b, (((0,), (0,)), ((), ())), preferred_element_type=f32)


def combine_tile(plan, tab, win_dst, win_chunks, lr, gt, tile, buf, out, gated):
    def piece(chunk):
        ones, gates = one_hot_rows(plan, tab, lr, gt, tile, chunk, not gated, gated)
        rows = jnp.concatenate([buf[win_rows(plan, win_dst, tile, chunk, i), :] for i in range(CHUNK)], 0)
        return dot_ta(gates if gated else ones, rows)

    total = piece(0)
    for chunk in range(1, MAIN):
        total = total + piece(chunk)
    span = pl.ds(pl.multiple_of(tile * TILE, TILE), TILE)
    out[span, :] = total

    def more(chunk, _):
        out[span, :] += piece(chunk)
        return 0

    lax.fori_loop(MAIN, jnp.maximum(win_chunks[tile], MAIN), more, 0)


def load_pieces(pieces, whole, sems, first):
    copies, row = [], 0
    for i, src in enumerate(pieces):
        copies.append(pltpu.make_async_copy(src, whole.at[pl.ds(row, src.shape[0])], sems.at[first + i]))
        row += src.shape[0]
    return copies


def load_weights(block, sources, targets, sems, first):
    return [pltpu.make_async_copy(src.at[0, block], dst, sems.at[first + i]) for i, (src, dst) in enumerate(zip(sources, targets))]


def chunks_of(win_chunks, tile, piece):
    for chunk in range(MAIN):
        piece(chunk)

    def more(chunk, _):
        piece(chunk)
        return 0

    lax.fori_loop(MAIN, jnp.maximum(win_chunks[tile], MAIN), more, 0)


def combine_all(plan, combine, y, outs, sems):
    size = outs[0].shape[0]
    sends = [pltpu.make_async_copy(y.at[pl.ds(i * size, size)], out, sems.at[i]) for i, out in enumerate(outs)]

    def step(i, _):
        tile = plan.tiles - 1 - i
        combine(tile, 0)
        for piece, send in enumerate(sends):
            pl.when(tile == piece * (size // TILE))(send.start)
        return 0

    lax.fori_loop(0, plan.tiles, step, 0)
    for send in sends:
        send.wait()


def forward_kernel(plan, block, win_exp, win_base, win_dst, win_chunks, exp_wins, lr, gt, z0, z1, z2, z3, wg_in, wu_in, wd_in, y0, y1, y2, y3, z, wg, wu, wd, buf, y, mid_a, mid_b, sems):
    ff = plan.ff
    loads = load_pieces((z0, z1, z2, z3), z, sems, 0)
    weights = load_weights(block, (wg_in, wu_in, wd_in), (wg, wu, wd), sems, 4)
    for load in loads + weights:
        load.start()
    tab = (win_exp, win_base)
    for load in loads:
        load.wait()

    def dispatch(tile, _):
        rows = z[pl.ds(pl.multiple_of(tile * TILE, TILE), TILE), :]

        def piece(chunk):
            ones, _ = one_hot_rows(plan, tab, lr, gt, tile, chunk, True, False)
            moved = dot(ones, rows).astype(bf16)
            for i in range(CHUNK):
                buf[win_rows(plan, win_dst, tile, chunk, i), :] = moved[i * WIN:(i + 1) * WIN, :]

        chunks_of(win_chunks, tile, piece)
        return 0

    lax.fori_loop(0, plan.tiles, dispatch, 0)
    for load in weights:
        load.wait()

    def span_of(exp, first):
        return pl.ds(pl.multiple_of(exp * plan.rows + first, TILE), TILE)

    def middle(exp, span):
        pre = dot(buf[span, :], jnp.concatenate([wg[exp], wu[exp]], 1))
        return (jax.nn.silu(pre[:, :ff]) * pre[:, ff:]).astype(bf16)

    def first_half(exp, mid):
        for i in range(2):
            mid[i * TILE:(i + 1) * TILE, :] = middle(exp, span_of(exp, i * TILE))

    def second_half(exp, mid):
        for i in range(2):
            buf[span_of(exp, i * TILE), :] = dot(mid[i * TILE:(i + 1) * TILE, :], wd[exp]).astype(bf16)

    def pair(step, _):
        exp = 2 * step
        first_half(exp + 1, mid_b)
        second_half(exp, mid_a)
        first_half(jnp.minimum(exp + 2, plan.experts - 1), mid_a)
        second_half(exp + 1, mid_b)
        return 0

    first_half(0, mid_a)
    lax.fori_loop(0, plan.experts // 2, pair, 0)

    def rest(exp, _):
        for first in range(2 * TILE, plan.rows, TILE):
            @pl.when(exp_wins[exp] * WIN > first)
            def _(first=first):
                span = span_of(exp, first)
                buf[span, :] = dot(middle(exp, span), wd[exp]).astype(bf16)
        return 0

    lax.fori_loop(0, plan.experts, rest, 0)

    def combine(tile, _):
        combine_tile(plan, tab, win_dst, win_chunks, lr, gt, tile, buf, y, True)
        return 0

    combine_all(plan, combine, y, (y0, y1, y2, y3), sems)


def backward_kernel(plan, block, n_g, n_out, aliased, *refs):
    win_exp, win_base, win_dst, win_chunks, exp_wins, lr, gt = refs[:7]
    z_in, g_in, w_src = refs[7:11], refs[11:11 + n_g], refs[11 + n_g:14 + n_g]
    refs = refs[14 + n_g + (3 if aliased else 0):]
    outs, (dwg, dwu, dwd) = refs[:n_out], refs[n_out:n_out + 3]
    z, g, wg, wu, wd, buf, rbuf, y, mid_a, mid_b, both_a, both_b, og, ou, od, sems, osems = refs[n_out + 3:]
    width, ff = plan.width, plan.ff
    loads = load_pieces(z_in, z, sems, 0) + load_pieces(g_in, g, sems, 4)
    weights = load_weights(block, w_src, (wg, wu, wd), sems, 4 + n_g)
    for load in loads + weights:
        load.start()
    tab = (win_exp, win_base)

    def clear(step, _):
        span = pl.ds(pl.multiple_of(step * TILE, TILE), TILE)
        buf[span, :] = jnp.zeros((TILE, width), bf16)
        rbuf[span, :] = jnp.zeros((TILE, width), bf16)
        return 0

    lax.fori_loop(0, plan.experts * plan.rows // TILE, clear, 0)
    for load in loads:
        load.wait()

    def dispatch(tile, _):
        span = pl.ds(pl.multiple_of(tile * TILE, TILE), TILE)
        z_rows, g_rows = z[span, :], g[span, :]

        def piece(chunk):
            ones, gates = one_hot_rows(plan, tab, lr, gt, tile, chunk, True, True)
            moved = dot(ones, z_rows).astype(bf16)
            sent = dot(gates, g_rows).astype(bf16)
            for i in range(CHUNK):
                dst = win_rows(plan, win_dst, tile, chunk, i)
                buf[dst, :] = moved[i * WIN:(i + 1) * WIN, :]
                rbuf[dst, :] = sent[i * WIN:(i + 1) * WIN, :]

        chunks_of(win_chunks, tile, piece)
        return 0

    lax.fori_loop(0, plan.tiles, dispatch, 0)
    for load in weights:
        load.wait()

    def span_of(exp, first):
        return pl.ds(pl.multiple_of(exp * plan.rows + first, TILE), TILE)

    def stores(exp, slot):
        return [pltpu.make_async_copy(src.at[slot], dst.at[block, exp], osems.at[slot, i]) for i, (src, dst) in enumerate(((og, dwg), (ou, dwu), (od, dwd)))]

    def in_weights(exp):
        return jnp.concatenate([wg[exp], wu[exp]], 1)

    def first_part(exp, first, mid, both, row):
        span = span_of(exp, first)
        pre = dot(buf[span, :], in_weights(exp))
        grad_mid = dot_tb(rbuf[span, :], wd[exp])
        gate_pre, up_pre = pre[:, :ff], pre[:, ff:]
        sig = jax.nn.sigmoid(gate_pre)
        act = gate_pre * sig
        mid[row:row + TILE, :] = (act * up_pre).astype(bf16)
        both[row:row + TILE, :ff] = (grad_mid * up_pre * (sig * (1.0 + gate_pre * (1.0 - sig)))).astype(bf16)
        both[row:row + TILE, ff:] = (grad_mid * act).astype(bf16)

    def second_part(exp, first, count, mid, both):
        spans = pl.ds(pl.multiple_of(exp * plan.rows + first, TILE), count)
        gu = dot_ta(buf[spans, :], both[0:count, :])
        down = dot_ta(mid[0:count, :], rbuf[spans, :])
        buf[spans, :] = dot_tb(both[0:count, :], in_weights(exp)).astype(bf16)
        return gu, down

    def first_half(exp, mid, both):
        for i in range(2):
            first_part(exp, i * TILE, mid, both, i * TILE)

    def second_half(exp, mid, both, slot, wait):
        @pl.when(wait)
        def _():
            for store in stores(exp, slot):
                store.wait()

        gu, down = second_part(exp, 0, 2 * TILE, mid, both)
        og[slot] = gu[:, :ff]
        ou[slot] = gu[:, ff:]
        od[slot] = down

    def send(exp, mid, both, slot):
        for first in range(2 * TILE, plan.rows, TILE):
            @pl.when(exp_wins[exp] * WIN > first)
            def _(first=first):
                first_part(exp, first, mid, both, 0)
                gu, down = second_part(exp, first, TILE, mid, both)
                og[slot] += gu[:, :ff]
                ou[slot] += gu[:, ff:]
                od[slot] += down

        for store in stores(exp, slot):
            store.start()

    def pair(step, _):
        exp = 2 * step
        first_half(exp + 1, mid_b, both_b)
        second_half(exp, mid_a, both_a, 0, step > 0)
        send(exp, mid_a, both_a, 0)
        first_half(jnp.minimum(exp + 2, plan.experts - 1), mid_a, both_a)
        second_half(exp + 1, mid_b, both_b, 1, step > 0)
        send(exp + 1, mid_b, both_b, 1)
        return 0

    first_half(0, mid_a, both_a)
    lax.fori_loop(0, plan.experts // 2, pair, 0)
    for slot in range(2):
        for store in stores(plan.experts - 2 + slot, slot):
            store.wait()

    def combine(tile, _):
        combine_tile(plan, tab, win_dst, win_chunks, lr, gt, tile, buf, y, False)
        return 0

    combine_all(plan, combine, y, outs, sems)


SMEM = pl.BlockSpec(memory_space=pltpu.SMEM)
VMEM = pl.BlockSpec(memory_space=pltpu.VMEM)
ANY = pl.BlockSpec(memory_space=pl.ANY)
LIMIT = 60 * 1024 * 1024


def weight_scratch(plan):
    e, d, f = plan.experts, plan.width, plan.ff
    return [pltpu.VMEM((e, d, f), bf16), pltpu.VMEM((e, d, f), bf16), pltpu.VMEM((e, f, d), bf16)]


def run_forward(plan, block, tables, z, weights):
    flops = 2 * plan.buf_rows * plan.width * plan.width * 4
    piece = jax.ShapeDtypeStruct((plan.n_tok, plan.width), f32)
    return pl.pallas_call(
        functools.partial(forward_kernel, plan, block),
        out_shape=(piece,) * 4,
        in_specs=[SMEM] * 5 + [VMEM] * 2 + [ANY] * 7,
        out_specs=(ANY,) * 4,
        scratch_shapes=[pltpu.VMEM((plan.total, plan.width), bf16)] + weight_scratch(plan) + [
            pltpu.VMEM((plan.buf_rows, plan.width), bf16),
            pltpu.VMEM((plan.total, plan.width), f32),
            pltpu.VMEM((2 * TILE, plan.ff), bf16),
            pltpu.VMEM((2 * TILE, plan.ff), bf16),
            pltpu.SemaphoreType.DMA((7,)),
        ],
        compiler_params=pltpu.CompilerParams(vmem_limit_bytes=LIMIT),
        cost_estimate=pl.CostEstimate(flops=flops, bytes_accessed=0, transcendentals=0),
        name="expert_forward",
    )(*tables, *z, *weights)


def run_backward(plan, block, tables, z, g, weights, grads, n_out):
    e, d, f = plan.experts, plan.width, plan.ff
    flops = 2 * plan.buf_rows * plan.width * plan.width * 8
    piece = jax.ShapeDtypeStruct((plan.total // n_out, plan.width), f32)
    up = jax.ShapeDtypeStruct((2, e, d, f), f32)
    down = jax.ShapeDtypeStruct((2, e, f, d), f32)
    n_g = len(g)
    return pl.pallas_call(
        functools.partial(backward_kernel, plan, block, n_g, n_out, bool(grads)),
        out_shape=(piece,) * n_out + (up, up, down),
        in_specs=[SMEM] * 5 + [VMEM] * 2 + [ANY] * (7 + n_g + len(grads)),
        out_specs=(ANY,) * (n_out + 3),
        scratch_shapes=[pltpu.VMEM((plan.total, plan.width), bf16)] * 2 + weight_scratch(plan) + [
            pltpu.VMEM((plan.buf_rows, plan.width), bf16),
            pltpu.VMEM((plan.buf_rows, plan.width), bf16),
            pltpu.VMEM((plan.total, plan.width), f32),
            pltpu.VMEM((2 * TILE, f), bf16),
            pltpu.VMEM((2 * TILE, f), bf16),
            pltpu.VMEM((2 * TILE, 2 * f), bf16),
            pltpu.VMEM((2 * TILE, 2 * f), bf16),
            pltpu.VMEM((2, d, f), f32),
            pltpu.VMEM((2, d, f), f32),
            pltpu.VMEM((2, f, d), f32),
            pltpu.SemaphoreType.DMA((15,)),
            pltpu.SemaphoreType.DMA((2, 3)),
        ],
        input_output_aliases={14 + n_g + i: n_out + i for i in range(len(grads))},
        compiler_params=pltpu.CompilerParams(vmem_limit_bytes=LIMIT),
        cost_estimate=pl.CostEstimate(flops=flops, bytes_accessed=0, transcendentals=0),
        name="expert_backward",
    )(*tables, *z, *g, *weights, *grads)


def solution(mesh):
    groups = mesh.shape['ep']
    stages = mesh.shape['pp']
    to_next = [(sender, (sender + 1) % stages) for sender in range(stages)]
    to_prev = [(sender, (sender - 1) % stages) for sender in range(stages)]
    core_pairs = [(dev, dev ^ 1) for dev in range(groups)]
    chip_pairs = [(dev, dev ^ 2) for dev in range(groups)]

    def swap_core(value):
        return lax.ppermute(value, 'ep', core_pairs)

    def swap_chip(value):
        return lax.ppermute(value, 'ep', chip_pairs)

    def local_step(x_fwd, x_bwd, grad_in, dense_in, dense_out, exp_gate, exp_up, exp_down, route_fwd, gate_fwd, route_bwd, gate_bwd):
        n_tok, width = x_fwd.shape[1], x_fwd.shape[2]
        choices = route_fwd.shape[3]
        experts, ff = exp_gate.shape[2], exp_gate.shape[4]
        plan = Plan(n_tok, groups, experts, choices, width, ff)
        capacity = 2 * n_tok * choices // (experts * groups)
        me = lax.axis_index('ep')

        def gather_rows(rows):
            far = swap_chip(rows)
            return rows, far, swap_core(rows), swap_core(far)

        def gather_halves(halves):
            parts = [gather_rows(rows) for rows in halves]
            return [half for piece in zip(*parts) for half in piece]

        def scatter_sum(y0, y1, y2, y3):
            far = swap_chip(y1 + swap_core(y3))
            return y0 + swap_core(y2) + far

        routes = jnp.concatenate([route_fwd[0], route_bwd[0]], 0)
        gates = jnp.concatenate([gate_fwd[0], gate_bwd[0]], 0)
        packed = jnp.stack([(routes // capacity).astype(bf16), gates]).transpose(0, 1, 3, 2)
        far = swap_chip(packed)
        mine = jnp.concatenate([packed, far], -1)
        whole = jnp.concatenate([mine, swap_core(mine)], -1)
        picks = whole[0].astype(jnp.int32) - me * experts
        gate_all = whole[1].astype(f32)
        match = picks[:, :, None, :] == jnp.arange(experts, dtype=jnp.int32)[None, None, :, None]
        chosen = jnp.sum(match.astype(f32), 1)
        gate_of = jnp.sum(jnp.where(match, gate_all[:, :, None, :], 0.0), 1)
        tiled = chosen.reshape(4, experts, plan.tiles, TILE)
        before = (jnp.arange(TILE)[:, None] < jnp.arange(TILE)[None, :]).astype(bf16)
        rank = jnp.einsum('qejt,ts->qejs', tiled.astype(bf16), before, preferred_element_type=f32)
        local_rank = jnp.where(tiled > 0, rank, -1.0).astype(jnp.int32).reshape(4, experts, plan.total)
        count = jnp.sum(tiled, -1).astype(jnp.int32)
        wins = (count + (WIN - 1)) // WIN
        in_tile = jnp.cumsum(wins, 1) - wins
        in_exp = jnp.cumsum(wins, 2) - wins
        tile_wins = jnp.sum(wins, 1)
        exp_wins = jnp.sum(wins, 2)
        spots = jnp.arange(plan.per_tile, dtype=jnp.int32)[None, None, :, None]
        start = in_tile.transpose(0, 2, 1)[:, :, None, :]
        size = wins.transpose(0, 2, 1)[:, :, None, :]
        owner = (spots >= start) & (spots < start + size)
        ids = jnp.arange(experts, dtype=jnp.int32)
        shift = (ids[None, :, None] * plan.per_exp + in_exp - in_tile).transpose(0, 2, 1)[:, :, None, :]
        used = jnp.any(owner, -1)
        win_exp = jnp.sum(jnp.where(owner, ids, 0), -1)
        win_base = jnp.where(used, jnp.sum(jnp.where(owner, (spots - start) * WIN, 0), -1), 1 << 20)
        win_dst = jnp.where(used, jnp.sum(jnp.where(owner, spots + shift, 0), -1), plan.trash)
        win_chunks = (tile_wins + (CHUNK - 1)) // CHUNK

        def tables(which):
            return (win_exp[which].reshape(-1), win_base[which].reshape(-1), win_dst[which].reshape(-1), win_chunks[which], exp_wins[which], local_rank[which], gate_of[which])

        weights = (exp_gate, exp_up, exp_down)

        def front(tokens, block):
            pre_act, hidden = dense_forward(tokens, dense_in[0, block], dense_out[0, block])
            normed = rms_norm(hidden.astype(f32)).astype(bf16)
            return pre_act, hidden, gather_rows(normed)

        def finish(hidden, rows, which, block):
            pieces = run_forward(plan, block, tables(which), rows, weights)
            return (hidden.astype(f32) + scatter_sum(*pieces)).astype(bf16)

        def through(grad_out, grad_norm, hidden, pre_act, tokens, block):
            grad_hidden = grad_out.astype(f32) + rms_back(hidden.astype(f32), grad_norm)
            return dense_backward(grad_hidden, tokens, pre_act, dense_in[0, block], dense_out[0, block])

        halves = [slice(0, n_tok // 2), slice(n_tok // 2, n_tok)]
        tok_b = x_bwd[0]
        pre_one, hid_one, rows_one = front(tok_b, 0)
        tok_f = x_fwd[0]
        _, hid_f, rows_f = front(tok_f, 0)
        grads_two = gather_rows(grad_in[0])
        mid_b = finish(hid_one, rows_one, 2, 0)
        pre_two, hid_two, rows_two = front(mid_b, 1)
        mid_f = finish(hid_f, rows_f, 0, 0)
        _, hid_g, rows_g = front(mid_f, 1)
        results = run_backward(plan, 1, tables(3), rows_two, grads_two, weights, (), 4)
        norm_two = scatter_sum(*results[:4])
        grad_mid = [through(grad_in[0][half], norm_two[half], hid_two[half], pre_two[half], mid_b[half], 1) for half in halves]
        out_f = finish(hid_g, rows_g, 1, 1)
        grads_one = gather_halves(grad_mid)
        results = run_backward(plan, 0, tables(2), rows_one, grads_one, weights, results[4:], 8)
        sums = results[8:]
        y_next = lax.ppermute(out_f, 'pp', to_next)
        shifted = []
        for i, half in enumerate(halves):
            norm_one = scatter_sum(*results[i:8:2])
            grad_first = through(grad_mid[i], norm_one, hid_one[half], pre_one[half], tok_b[half], 0)
            shifted.append(lax.ppermute(grad_first, 'pp', to_prev))
        dx_prev = jnp.concatenate(shifted, 0)
        return (y_next[None], dx_prev[None], sums[0][None], sums[1][None], sums[2][None])

    tok_spec = P('pp', 'ep', None)
    dense_spec = P('pp', None, None, None)
    exp_spec = P('pp', None, 'ep', None, None)
    route_spec = P('pp', None, 'ep', None)
    return jax.shard_map(local_step, mesh=mesh, in_specs=(tok_spec, tok_spec, tok_spec, dense_spec, dense_spec, exp_spec, exp_spec, exp_spec, route_spec, route_spec, route_spec, route_spec), out_specs=(tok_spec, tok_spec, exp_spec, exp_spec, exp_spec), check_vma=False)
```

```python
import functools

import jax
import jax.numpy as jnp
from jax import lax
from jax.experimental import pallas as pl
from jax.experimental.pallas import tpu as pltpu
from jax.sharding import PartitionSpec as P


NORM_EPS = 1e-6
WIN = 16
TILE = 256
CHUNK = 16
MAIN = 4

f32 = jnp.float32
bf16 = jnp.bfloat16


def rms_norm(values):
    return values * lax.rsqrt(jnp.mean(values * values, axis=-1, keepdims=True) + NORM_EPS)


def rms_back(values, grad_out):
    inv_rms = lax.rsqrt(jnp.mean(values * values, axis=-1, keepdims=True) + NORM_EPS)
    proj_mean = jnp.mean(grad_out * values, axis=-1, keepdims=True)
    return inv_rms * grad_out - values * (inv_rms * inv_rms * inv_rms) * proj_mean


def silu_grad(pre_act):
    sig_value = jax.nn.sigmoid(pre_act)
    return sig_value * (1.0 + pre_act * (1.0 - sig_value))


def dense_forward(tokens, w_in, w_out):
    normed = rms_norm(tokens.astype(f32)).astype(bf16)
    pre_act = jnp.dot(normed, w_in, preferred_element_type=f32)
    mid_act = jax.nn.silu(pre_act).astype(bf16)
    hidden = (tokens.astype(f32) + jnp.dot(mid_act, w_out, preferred_element_type=f32)).astype(bf16)
    return pre_act, hidden


def dense_backward(grad_hidden, tokens, pre_act, w_in, w_out):
    grad_dense = jnp.einsum('td,fd->tf', grad_hidden.astype(bf16), w_out, preferred_element_type=f32)
    grad_pre = (grad_dense * silu_grad(pre_act)).astype(bf16)
    grad_act = jnp.einsum('tf,df->td', grad_pre, w_in, preferred_element_type=f32)
    return (grad_hidden + rms_back(tokens.astype(f32), grad_act)).astype(bf16)


class Plan:
    def __init__(self, n_tok, groups, experts, choices, width, ff):
        self.n_tok, self.groups, self.experts, self.width, self.ff = n_tok, groups, experts, width, ff
        self.total = n_tok * groups
        self.tiles = self.total // TILE
        capacity = 2 * n_tok * choices // (experts * groups)
        worst = (TILE * choices + experts * (WIN - 1)) // WIN
        self.per_tile = -(-worst // CHUNK) * CHUNK
        self.per_exp = -(-(groups * capacity + self.tiles * (WIN - 1)) // (WIN * 16)) * 16
        self.rows = self.per_exp * WIN
        self.trash = experts * self.per_exp
        self.buf_rows = (self.trash + 1) * WIN


def one_hot_rows(spots, picks, tile, chunk, plain, gated):
    span = pl.ds(pl.multiple_of(chunk * CHUNK, CHUNK), CHUNK)
    spot = spots[tile, span, :].astype(f32)
    pick = picks[tile, span, :].astype(f32) if gated else None
    place = (lax.broadcasted_iota(jnp.int32, (WIN, TILE), 0) + 1).astype(f32)
    ones, gates = [], []
    for i in range(CHUNK):
        hit = spot[i:i + 1, :] == place
        if plain:
            ones.append(jnp.where(hit, 1.0, 0.0).astype(bf16))
        if gated:
            gates.append(jnp.where(hit, pick[i:i + 1, :], 0.0).astype(bf16))
    return (jnp.concatenate(ones, 0) if plain else None), (jnp.concatenate(gates, 0) if gated else None)


def win_rows(win_dst, tile, chunk, i):
    return pl.ds(pl.multiple_of(win_dst[tile, chunk * CHUNK + i], WIN), WIN)


def dot(a, b):
    return jnp.dot(a, b, preferred_element_type=f32)


def dot_tb(a, b):
    return lax.dot_general(a, b, (((1,), (1,)), ((), ())), preferred_element_type=f32)


def dot_ta(a, b):
    return lax.dot_general(a, b, (((0,), (0,)), ((), ())), preferred_element_type=f32)


def tile_rows(tile):
    return pl.ds(pl.multiple_of(tile * TILE, TILE), TILE)


def load_pieces(pieces, whole, sems, first):
    copies, row = [], 0
    for i, src in enumerate(pieces):
        copies.append(pltpu.make_async_copy(src, whole.at[pl.ds(row, src.shape[0])], sems.at[first + i]))
        row += src.shape[0]
    return copies


def load_weights(block, sources, targets, sems, first):
    return [pltpu.make_async_copy(src.at[0, block], dst, sems.at[first + i]) for i, (src, dst) in enumerate(zip(sources, targets))]


def all_chunks(plan, win_chunks, main, piece, ahead=None):
    def more(tile, _):
        def one(chunk, _):
            piece(tile, chunk)
            return 0

        lax.fori_loop(MAIN, jnp.maximum(win_chunks[0, tile], MAIN), one, 0)
        return 0

    def step(i, _):
        tile = plan.tiles - 2 - 2 * i
        main(tile + 1)
        main(tile)
        if ahead is not None:
            lax.fori_loop(tile, tile + 2, more, 0)
            ahead(tile)
        return 0

    lax.fori_loop(0, plan.tiles // 2, step, 0)
    if ahead is None:
        lax.fori_loop(0, plan.tiles, more, 0)


def combine_all(plan, spots, picks, win_dst, win_chunks, buf, gated, y, outs, sems):
    size = outs[0].shape[0]
    sends = [pltpu.make_async_copy(y.at[pl.ds(i * size, size)], out, sems.at[i]) for i, out in enumerate(outs)]

    def product(tile, chunk):
        ones, gates = one_hot_rows(spots, picks, tile, chunk, not gated, gated)
        rows = jnp.concatenate([buf[win_rows(win_dst, tile, chunk, i), :] for i in range(CHUNK)], 0)
        return dot_ta(gates if gated else ones, rows)

    def main(tile):
        total = product(tile, 0)
        for chunk in range(1, MAIN):
            total = total + product(tile, chunk)
        y[tile_rows(tile), :] = total

    def piece(tile, chunk):
        y[tile_rows(tile), :] += product(tile, chunk)

    def ahead(tile):
        for i, send in enumerate(sends):
            pl.when(tile == i * (size // TILE))(send.start)

    all_chunks(plan, win_chunks, main, piece, ahead)
    for send in sends:
        send.wait()


def forward_kernel(plan, block, n_z, *refs):
    win_dst, win_chunks, exp_wins, spots_in, picks_in = refs[:5]
    z_in, w_src, outs = refs[5:5 + n_z], refs[5 + n_z:8 + n_z], refs[8 + n_z:12 + n_z]
    spots, picks, z, wg, wu, wd, buf, y, mid_a, mid_b, sems = refs[12 + n_z:]
    ff = plan.ff
    loads = [pltpu.make_async_copy(spots_in, spots, sems.at[n_z + 3])] + load_pieces(z_in, z, sems, 0)
    weights = load_weights(block, w_src, (wg, wu, wd), sems, n_z)
    weights.append(pltpu.make_async_copy(picks_in, picks, sems.at[n_z + 4]))
    for load in loads + weights:
        load.start()
    for load in loads:
        load.wait()

    def piece(tile, chunk):
        ones, _ = one_hot_rows(spots, picks, tile, chunk, True, False)
        moved = dot(ones, z[tile_rows(tile), :]).astype(bf16)
        for i in range(CHUNK):
            buf[win_rows(win_dst, tile, chunk, i), :] = moved[i * WIN:(i + 1) * WIN, :]

    def main(tile):
        for chunk in range(MAIN):
            piece(tile, chunk)

    all_chunks(plan, win_chunks, main, piece)
    for load in weights:
        load.wait()

    def span_of(exp, first):
        return pl.ds(pl.multiple_of(exp * plan.rows + first, TILE), TILE)

    def middle(exp, span):
        pre = dot(buf[span, :], jnp.concatenate([wg[exp], wu[exp]], 1))
        return (jax.nn.silu(pre[:, :ff]) * pre[:, ff:]).astype(bf16)

    def first_half(exp, mid):
        for i in range(2):
            mid[i * TILE:(i + 1) * TILE, :] = middle(exp, span_of(exp, i * TILE))

    def second_half(exp, mid):
        for i in range(2):
            buf[span_of(exp, i * TILE), :] = dot(mid[i * TILE:(i + 1) * TILE, :], wd[exp]).astype(bf16)

    def pair(step, _):
        exp = 2 * step
        first_half(exp + 1, mid_b)
        second_half(exp, mid_a)
        first_half(jnp.minimum(exp + 2, plan.experts - 1), mid_a)
        second_half(exp + 1, mid_b)
        return 0

    first_half(0, mid_a)
    lax.fori_loop(0, plan.experts // 2, pair, 0)

    def rest(exp, _):
        for first in range(2 * TILE, plan.rows, TILE):
            @pl.when(exp_wins[exp, 0] * WIN > first)
            def _(first=first):
                span = span_of(exp, first)
                buf[span, :] = dot(middle(exp, span), wd[exp]).astype(bf16)
        return 0

    lax.fori_loop(0, plan.experts, rest, 0)

    combine_all(plan, spots, picks, win_dst, win_chunks, buf, True, y, outs, sems)


def backward_kernel(plan, block, n_z, n_in, n_out, aliased, *refs):
    win_dst, win_chunks, exp_wins, spots_in, picks_in = refs[:5]
    z_in, g_in, w_src = refs[5:5 + n_z], refs[5 + n_z:5 + n_in], refs[5 + n_in:8 + n_in]
    refs = refs[8 + n_in + (3 if aliased else 0):]
    outs, (dwg, dwu, dwd) = refs[:n_out], refs[n_out:n_out + 3]
    spots, picks, z, g, wg, wu, wd, buf, rbuf, y, mid_a, mid_b, mid_c, both_a, both_b, both_c, og, ou, od, sems, osems = refs[n_out + 3:]
    width, ff = plan.width, plan.ff
    loads = [pltpu.make_async_copy(spots_in, spots, sems.at[n_in + 3]), pltpu.make_async_copy(picks_in, picks, sems.at[n_in + 4])]
    loads += load_pieces(z_in, z, sems, 0) + load_pieces(g_in, g, sems, n_z)
    weights = load_weights(block, w_src, (wg, wu, wd), sems, n_in)
    for load in loads + weights:
        load.start()

    def clear(step, _):
        span = tile_rows(step)
        buf[span, :] = jnp.zeros((TILE, width), bf16)
        rbuf[span, :] = jnp.zeros((TILE, width), bf16)
        return 0

    lax.fori_loop(0, plan.experts * plan.rows // TILE, clear, 0)
    for load in loads:
        load.wait()

    def piece(tile, chunk):
        span = tile_rows(tile)
        ones, gates = one_hot_rows(spots, picks, tile, chunk, True, True)
        moved = dot(ones, z[span, :]).astype(bf16)
        sent = dot(gates, g[span, :]).astype(bf16)
        for i in range(CHUNK):
            dst = win_rows(win_dst, tile, chunk, i)
            buf[dst, :] = moved[i * WIN:(i + 1) * WIN, :]
            rbuf[dst, :] = sent[i * WIN:(i + 1) * WIN, :]

    def main(tile):
        for chunk in range(MAIN):
            piece(tile, chunk)

    all_chunks(plan, win_chunks, main, piece)
    for load in weights:
        load.wait()

    def span_of(exp, first):
        return pl.ds(pl.multiple_of(exp * plan.rows + first, TILE), TILE)

    def stores(exp, slot):
        return [pltpu.make_async_copy(src.at[slot], dst.at[block, exp], osems.at[slot, i]) for i, (src, dst) in enumerate(((og, dwg), (ou, dwu), (od, dwd)))]

    def in_weights(exp):
        return jnp.concatenate([wg[exp], wu[exp]], 1)

    def first_part(exp, first, mid, both, row):
        span = span_of(exp, first)
        pre = dot(buf[span, :], in_weights(exp))
        grad_mid = dot_tb(rbuf[span, :], wd[exp])
        gate_pre, up_pre = pre[:, :ff], pre[:, ff:]
        sig = jax.nn.sigmoid(gate_pre)
        act = gate_pre * sig
        mid[row:row + TILE, :] = (act * up_pre).astype(bf16)
        both[row:row + TILE, :ff] = (grad_mid * up_pre * (sig * (1.0 + gate_pre * (1.0 - sig)))).astype(bf16)
        both[row:row + TILE, ff:] = (grad_mid * act).astype(bf16)

    def second_part(exp, first, count, mid, both):
        spans = pl.ds(pl.multiple_of(exp * plan.rows + first, TILE), count)
        gu = dot_ta(buf[spans, :], both[0:count, :])
        down = dot_ta(mid[0:count, :], rbuf[spans, :])
        buf[spans, :] = dot_tb(both[0:count, :], in_weights(exp)).astype(bf16)
        return gu, down

    def first_half(exp, mid, both):
        for i in range(2):
            first_part(exp, i * TILE, mid, both, i * TILE)

    def second_half(exp, mid, both, slot):
        gu, down = second_part(exp, 0, 2 * TILE, mid, both)
        og[slot] = gu[:, :ff]
        ou[slot] = gu[:, ff:]
        od[slot] = down

    def extra(slot, i, exp):
        for first in range(2 * TILE, plan.rows, TILE):
            @pl.when(exp_wins[exp + i, 0] * WIN > first)
            def _(first=first):
                first_part(exp + i, first, mid_c, both_c, 0)
                gu, down = second_part(exp + i, first, TILE, mid_c, both_c)
                og[slot + i] += gu[:, :ff]
                ou[slot + i] += gu[:, ff:]
                od[slot + i] += down
        return exp

    def pair(step, _):
        exp = 2 * step
        slot = 2 * lax.rem(step, 2)

        @pl.when(step > 1)
        def _():
            for i in range(2):
                for store in stores(exp + i, slot + i):
                    store.wait()

        first_half(exp + 1, mid_b, both_b)
        second_half(exp, mid_a, both_a, slot)
        first_half(jnp.minimum(exp + 2, plan.experts - 1), mid_a, both_a)
        second_half(exp + 1, mid_b, both_b, slot + 1)
        lax.fori_loop(0, 2, functools.partial(extra, slot), exp)
        for i in range(2):
            for store in stores(exp + i, slot + i):
                store.start()
        return 0

    first_half(0, mid_a, both_a)
    lax.fori_loop(0, plan.experts // 2, pair, 0)
    for slot in range(4):
        for store in stores(slot, slot):
            store.wait()

    combine_all(plan, spots, picks, win_dst, win_chunks, buf, False, y, outs, sems)


SPOTS = 256


def table_kernel(plan, capacity, *refs):
    experts = plan.experts
    per_src = plan.n_tok // TILE
    routes, gates, outs = refs[:plan.groups], refs[plan.groups:2 * plan.groups], refs[2 * plan.groups:-2]
    ranks, weights = refs[-2:]
    first = lax.axis_index('ep') * experts

    def iota(shape, axis):
        return lax.broadcasted_iota(jnp.int32, shape, axis)

    def mask(hit):
        return jnp.where(hit, 1.0, 0.0).astype(bf16)

    before = mask(iota((TILE, TILE), 0) <= iota((TILE, TILE), 1))
    above = mask(iota((experts, experts), 1) < iota((experts, experts), 0))
    left = mask(iota((128, 128), 0) < iota((128, 128), 1))
    exp_id = iota((experts, TILE), 0)
    exp_f = iota((experts, SPOTS), 0).astype(f32)
    spot = iota((experts, SPOTS), 1).astype(f32)
    ones = jnp.ones((experts, TILE), bf16)
    for block in range(2):
        win_dst, win_chunks, exp_wins, spots, picks = outs[5 * block:5 * block + 5]
        counts = jnp.zeros((experts, 128), f32)
        for tile in range(plan.tiles):
            src, lane = tile // per_src, pl.ds(tile % per_src * TILE, TILE)
            here = slice(tile * TILE, (tile + 1) * TILE)
            pick = lax.div(routes[src][block, :, lane], capacity) - first
            gate = gates[src][block, :, lane].astype(f32)
            chosen = jnp.zeros((experts, TILE), f32)
            weight = jnp.zeros((experts, TILE), f32)
            for k in range(pick.shape[0]):
                hit = pick[k:k + 1, :] == exp_id
                chosen = jnp.where(hit, 1.0, chosen)
                weight = jnp.where(hit, gate[k:k + 1, :], weight)
            rank = dot(chosen.astype(bf16), before)
            ranks[:, here] = (rank * chosen).astype(bf16)
            weights[:, here] = weight.astype(bf16)
            counts = jnp.where(iota((experts, 128), 1) == tile, jnp.sum(chosen, 1, keepdims=True), counts)
        wins = jnp.floor((counts + (WIN - 1)) * (1.0 / WIN))
        in_tile = dot(above, wins.astype(bf16))
        in_exp = dot(wins.astype(bf16), left)
        chunk_count = jnp.floor((jnp.sum(wins, 0, keepdims=True) + (CHUNK - 1)) * (1.0 / CHUNK))
        win_chunks[...] = jnp.broadcast_to(chunk_count, (8, 128)).astype(jnp.int32)
        exp_wins[...] = jnp.broadcast_to(jnp.sum(wins, 1, keepdims=True), (experts, 128)).astype(jnp.int32)
        for tile in range(plan.tiles):
            here = slice(tile * TILE, (tile + 1) * TILE)
            rel = spot - in_tile[:, tile:tile + 1]
            own = (rel >= 0) & (rel < wins[:, tile:tile + 1])
            used = jnp.sum(jnp.where(own, 1.0, 0.0), 0, keepdims=True) > 0
            place = exp_f * plan.per_exp + in_exp[:, tile:tile + 1] + rel
            dst = jnp.sum(jnp.where(own, place, 0.0), 0, keepdims=True)
            win_dst[tile:tile + 1, :] = jnp.where(used, dst * WIN, float(plan.trash * WIN)).astype(jnp.int32)
            owner = mask(own)
            offset = jnp.where(own, rel * -WIN, 0.0).astype(bf16)
            moved = dot_ta(jnp.concatenate([owner, offset], 0), jnp.concatenate([ranks[:, here], ones], 0))
            spots[tile] = moved[:plan.per_tile, :].astype(bf16)
            picks[tile] = dot_ta(owner, weights[:, here])[:plan.per_tile, :].astype(bf16)


SMEM = pl.BlockSpec(memory_space=pltpu.SMEM)
WHOLE = pl.BlockSpec()
ANY = pl.BlockSpec(memory_space=pl.ANY)
LIMIT = 60 * 1024 * 1024


def weight_scratch(plan):
    e, d, f = plan.experts, plan.width, plan.ff
    return [pltpu.VMEM((e, d, f), bf16), pltpu.VMEM((e, d, f), bf16), pltpu.VMEM((e, f, d), bf16)]


def table_scratch(plan):
    return [pltpu.VMEM((plan.tiles, plan.per_tile, TILE), bf16)] * 2


def run_tables(plan, capacity, routes, gates):
    i32 = jnp.int32
    moves = jax.ShapeDtypeStruct((plan.tiles, plan.per_tile, TILE), bf16)
    shapes = (jax.ShapeDtypeStruct((plan.tiles, SPOTS), i32), jax.ShapeDtypeStruct((8, 128), i32),
              jax.ShapeDtypeStruct((plan.experts, 128), i32), moves, moves)
    tables = pl.pallas_call(
        functools.partial(table_kernel, plan, capacity),
        out_shape=shapes * 2,
        in_specs=[WHOLE] * (2 * plan.groups),
        out_specs=(WHOLE,) * 10,
        scratch_shapes=[pltpu.VMEM((plan.experts, plan.total), bf16)] * 2,
        compiler_params=pltpu.CompilerParams(vmem_limit_bytes=LIMIT),
        cost_estimate=pl.CostEstimate(flops=10 ** 9, bytes_accessed=0, transcendentals=0),
        name="window_tables",
    )(*routes, *gates)
    return tables[:5], tables[5:]


def run_forward(plan, block, tables, z, weights):
    flops = 2 * plan.buf_rows * plan.width * plan.width * 4
    piece = jax.ShapeDtypeStruct((plan.n_tok, plan.width), f32)
    return pl.pallas_call(
        functools.partial(forward_kernel, plan, block, len(z)),
        out_shape=(piece,) * 4,
        in_specs=[SMEM] * 3 + [ANY] * (5 + len(z)),
        out_specs=(ANY,) * 4,
        scratch_shapes=table_scratch(plan) + [pltpu.VMEM((plan.total, plan.width), bf16)] + weight_scratch(plan) + [
            pltpu.VMEM((plan.buf_rows, plan.width), bf16),
            pltpu.VMEM((plan.total, plan.width), f32),
            pltpu.VMEM((2 * TILE, plan.ff), bf16),
            pltpu.VMEM((2 * TILE, plan.ff), bf16),
            pltpu.SemaphoreType.DMA((13,)),
        ],
        compiler_params=pltpu.CompilerParams(vmem_limit_bytes=LIMIT),
        cost_estimate=pl.CostEstimate(flops=flops, bytes_accessed=0, transcendentals=0),
        name="expert_forward",
    )(*tables, *z, *weights)


def run_backward(plan, block, tables, z, g, weights, grads, n_out):
    e, d, f = plan.experts, plan.width, plan.ff
    flops = 2 * plan.buf_rows * plan.width * plan.width * 8
    piece = jax.ShapeDtypeStruct((plan.total // n_out, plan.width), f32)
    up = jax.ShapeDtypeStruct((2, e, d, f), f32)
    down = jax.ShapeDtypeStruct((2, e, f, d), f32)
    n_in = len(z) + len(g)
    return pl.pallas_call(
        functools.partial(backward_kernel, plan, block, len(z), n_in, n_out, bool(grads)),
        out_shape=(piece,) * n_out + (up, up, down),
        in_specs=[SMEM] * 3 + [ANY] * (5 + n_in + len(grads)),
        out_specs=(ANY,) * (n_out + 3),
        scratch_shapes=table_scratch(plan) + [pltpu.VMEM((plan.total, plan.width), bf16)] * 2 + weight_scratch(plan) + [
            pltpu.VMEM((plan.buf_rows, plan.width), bf16),
            pltpu.VMEM((plan.buf_rows, plan.width), bf16),
            pltpu.VMEM((plan.total, plan.width), f32),
            pltpu.VMEM((2 * TILE, f), bf16),
            pltpu.VMEM((2 * TILE, f), bf16),
            pltpu.VMEM((TILE, f), bf16),
            pltpu.VMEM((2 * TILE, 2 * f), bf16),
            pltpu.VMEM((2 * TILE, 2 * f), bf16),
            pltpu.VMEM((TILE, 2 * f), bf16),
            pltpu.VMEM((4, d, f), f32),
            pltpu.VMEM((4, d, f), f32),
            pltpu.VMEM((4, f, d), f32),
            pltpu.SemaphoreType.DMA((21,)),
            pltpu.SemaphoreType.DMA((4, 3)),
        ],
        input_output_aliases={8 + n_in + i: n_out + i for i in range(len(grads))},
        compiler_params=pltpu.CompilerParams(vmem_limit_bytes=LIMIT),
        cost_estimate=pl.CostEstimate(flops=flops, bytes_accessed=0, transcendentals=0),
        name="expert_backward",
    )(*tables, *z, *g, *weights, *grads)


def join_kernel(first, second, out):
    half = first.shape[0]
    out[:half, :] = first[...]
    out[half:, :] = second[...]


def join_halves(first, second):
    out = jax.ShapeDtypeStruct((2 * first.shape[0], first.shape[1]), first.dtype)
    return pl.pallas_call(join_kernel, out_shape=out, compiler_params=pltpu.CompilerParams(vmem_limit_bytes=LIMIT), name="join_halves")(first, second)


def solution(mesh):
    groups = mesh.shape['ep']
    stages = mesh.shape['pp']
    to_next = [(sender, (sender + 1) % stages) for sender in range(stages)]
    to_prev = [(sender, (sender - 1) % stages) for sender in range(stages)]
    core_pairs = [(dev, dev ^ 1) for dev in range(groups)]
    chip_pairs = [(dev, dev ^ 2) for dev in range(groups)]

    def swap_core(value):
        return lax.ppermute(value, 'ep', core_pairs)

    def swap_chip(value):
        return lax.ppermute(value, 'ep', chip_pairs)

    def local_step(x_fwd, x_bwd, grad_in, dense_in, dense_out, exp_gate, exp_up, exp_down, route_fwd, gate_fwd, route_bwd, gate_bwd):
        n_tok, width = x_fwd.shape[1], x_fwd.shape[2]
        choices = route_fwd.shape[3]
        experts, ff = exp_gate.shape[2], exp_gate.shape[4]
        plan = Plan(n_tok, groups, experts, choices, width, ff)
        capacity = 2 * n_tok * choices // (experts * groups)

        def gather_rows(rows):
            far = swap_chip(rows)
            return rows, far, swap_core(rows), swap_core(far)

        def gather_halves(halves):
            parts = [gather_rows(rows) for rows in halves]
            return [half for piece in zip(*parts) for half in piece]

        def scatter_sum(y0, y1, y2, y3):
            pair = y1 + swap_core(y3)
            far = swap_chip(pair)
            return y0 + swap_core(y2) + far

        def tables_of(route, gate):
            routes = gather_rows(route[0].transpose(0, 2, 1))
            gates = gather_rows(gate[0].transpose(0, 2, 1))
            return run_tables(plan, capacity, routes, gates)

        tables_b = tables_of(route_bwd, gate_bwd)
        tables_f = tables_of(route_fwd, gate_fwd)
        tables = (*tables_f, *tables_b)

        weights = (exp_gate, exp_up, exp_down)

        halves = [slice(0, n_tok // 2), slice(n_tok // 2, n_tok)]

        def normed_of(tokens, block):
            pre_act, hidden = dense_forward(tokens, dense_in[0, block], dense_out[0, block])
            return pre_act, hidden, rms_norm(hidden.astype(f32)).astype(bf16)

        def front(tokens, block):
            pre_act, hidden, normed = normed_of(tokens, block)
            return pre_act, hidden, gather_rows(normed)

        def front_halves(tokens, block):
            first, second = tokens[halves[0]], tokens[halves[1]]
            pre_a, hid_a, norm_a = normed_of(first, block)
            norm_a, second = lax.optimization_barrier((norm_a, second))
            pre_b, hid_b, norm_b = normed_of(second, block)
            return (pre_a, pre_b), (hid_a, hid_b), gather_halves([norm_a, norm_b]), (first, second)

        def finish(hidden, rows, which, block):
            pieces = run_forward(plan, block, tables[which], rows, weights)
            return (hidden.astype(f32) + scatter_sum(*pieces)).astype(bf16)

        def through(grad_out, grad_norm, hidden, pre_act, tokens, block):
            grad_hidden = grad_out.astype(f32) + rms_back(hidden.astype(f32), grad_norm)
            return dense_backward(grad_hidden, tokens, pre_act, dense_in[0, block], dense_out[0, block])

        tok_b = x_bwd[0]
        pre_one, hid_one, rows_one = front(tok_b, 0)
        tok_f = x_fwd[0]
        _, hid_f, rows_f = front(tok_f, 0)
        grads_two = gather_rows(grad_in[0])
        mid_b = finish(hid_one, rows_one, 2, 0)
        pre_two, hid_two, rows_two, mid_two = front_halves(mid_b, 1)
        mid_f = finish(hid_f, rows_f, 0, 0)
        _, hid_g, rows_g, _ = front_halves(mid_f, 1)
        results = run_backward(plan, 1, tables[3], rows_two, grads_two, weights, (), 4)
        norm_two = scatter_sum(*results[:4])
        norm_a, norm_b = norm_two[halves[0]], norm_two[halves[1]]
        grad_a = through(grad_in[0][halves[0]], norm_a, hid_two[0], pre_two[0], mid_two[0], 1)
        grad_a, hid_b = lax.optimization_barrier((grad_a, hid_two[1]))
        grad_b = through(grad_in[0][halves[1]], norm_b, hid_b, pre_two[1], mid_two[1], 1)
        out_f = finish(jnp.concatenate(hid_g, 0), rows_g, 1, 1)
        grads_one = gather_halves([grad_a, grad_b])
        results = run_backward(plan, 0, tables[2], rows_one, grads_one, weights, results[4:], 8)
        sums = results[8:]
        y_next = lax.ppermute(out_f, 'pp', to_next)
        norm_a = scatter_sum(*results[0:8:2])
        norm_b = scatter_sum(*results[1:8:2])
        last_a = through(grad_a, norm_a, hid_one[halves[0]], pre_one[halves[0]], tok_b[halves[0]], 0)
        last_a, norm_b = lax.optimization_barrier((last_a, norm_b))
        last_b = through(grad_b, norm_b, hid_one[halves[1]], pre_one[halves[1]], tok_b[halves[1]], 0)
        last_a = lax.ppermute(last_a, 'pp', to_prev)
        last_b = lax.ppermute(last_b, 'pp', to_prev)
        dx_prev = join_halves(last_a, last_b)
        return (y_next[None], dx_prev[None], sums[0][None], sums[1][None], sums[2][None])

    tok_spec = P('pp', 'ep', None)
    dense_spec = P('pp', None, None, None)
    exp_spec = P('pp', None, 'ep', None, None)
    route_spec = P('pp', None, 'ep', None)
    return jax.shard_map(local_step, mesh=mesh, in_specs=(tok_spec, tok_spec, tok_spec, dense_spec, dense_spec, exp_spec, exp_spec, exp_spec, route_spec, route_spec, route_spec, route_spec), out_specs=(tok_spec, tok_spec, exp_spec, exp_spec, exp_spec), check_vma=False)
```
